32 devices in a mesh: row: 8 (over y, x, core), col: 4 (over z).
Axes of the slice: x: 2, y: 2, z: 4, core: 2. Of those that a mesh axis runs over, the one named last changes fastest.
Arguments:
- singular_vectors: float32 [4096, 4096], P('row', 'col'), may hold values from -6 to 6
- reflector_vectors: float32 [2, 16, 256, 512], P(None, 'row', 'col'), may hold values from -2 to 2, as said below
- reflector_factors: float32 [2, 16, 256, 256], P(None, 'row', 'col'), as said below
- sweep_bounds: int32 [2, 2], replicated, may hold values from 0 to 3584, as said below
Outputs:
- transformed: float32 [4096, 4096], P('row', 'col')
The draws below stay inside these ranges and needn't reach their ends.
Inputs may be any that keep to these rules, and one draw needn't show every extreme that they name: `reflector_vectors`: row j of each block's 256 x 2 * 256 slice is a reflector: 1 at position j, nonzero only at positions j to j + 255. `reflector_factors`: each block's factor is the upper triangular inverse of the strictly upper part of W W^T plus half of its diagonal, W being that block's slice of reflector_vectors, so that each block's transformation is orthogonal. `sweep_bounds`: both entries are multiples of 256, and the first is below the second.
All inputs are finite; a program needn't handle non-finite values.
Results may differ from the reference program's by a relative error of at most 0.0003.
Values sent between devices are 32-bit elements; how exact they have to be, the bound alone decides.
A program may use at most 64 MiB of HBM per device.

```python
import jax
import jax.numpy as jnp
from jax import lax

BW = 256
NV = 4096
SWEEPS = 2
ROWS = 4096
BLOCKS = 16


exact_mode = lax.Precision.HIGHEST


def build_factor(vectors):
    gram = jnp.dot(vectors, vectors.T, precision=exact_mode, preferred_element_type=jnp.float32)
    upper = jnp.triu(gram, 1) + jnp.diag(0.5 * jnp.diagonal(gram))
    identity = jnp.eye(gram.shape[0], dtype=jnp.float32)
    return lax.linalg.triangular_solve(upper, identity, left_side=True, lower=False)


def reflector_pair(key):
    base_key = jax.random.fold_in(key, 11)
    tail_scale = 0.25 / BW ** 0.5
    noise = jax.random.truncated_normal(base_key, -4.0, 4.0, (SWEEPS, BLOCKS, BW, 2 * BW), jnp.float32)
    column = lax.broadcasted_iota(jnp.int32, (BW, 2 * BW), 1)
    reflector_row = lax.broadcasted_iota(jnp.int32, (BW, 2 * BW), 0)
    tail_mask = (column > reflector_row) & (column < reflector_row + BW)
    head_mask = column == reflector_row
    far_mask = column == reflector_row + BW - 1
    vectors = jnp.where(tail_mask, noise * tail_scale, 0.0) + jnp.where(head_mask, 1.0, 0.0) + jnp.where(far_mask, 1.0, 0.0)
    vectors = vectors.astype(jnp.float32)
    factors = jax.vmap(jax.vmap(build_factor))(vectors)
    return (vectors, factors)


def draw_reflector_vectors(key, part):
    return reflector_pair(key)[0]


def draw_reflector_factors(key, part):
    return reflector_pair(key)[1]


def draw_sweep_bounds(key, part):
    first_key = jax.random.fold_in(key, 21)
    last_key = jax.random.fold_in(key, 22)
    first_row = jax.random.randint(first_key, (SWEEPS,), 0, BLOCKS // 4) * BW
    last_row = jax.random.randint(last_key, (SWEEPS,), BLOCKS * 3 // 4 - 1, BLOCKS - 1) * BW
    return jnp.stack([first_row, last_row], axis=1).astype(jnp.int32)


def steps_of(own_key, dims, pieces, smallest, largest):
    level, own = 1.0, jax.random.fold_in(own_key, 6)
    for axis_at, shards_of in pieces:
        heights = jnp.exp(jax.random.uniform(jax.random.fold_in(own, axis_at), (shards_of,), jnp.float32, smallest / len(pieces), largest / len(pieces)))
        level = level * jnp.repeat(heights, dims[axis_at] // shards_of).reshape([-1 if axis == axis_at else 1 for axis in range(len(dims))])
    return level


def centred(stream_key, shape, deviation, most, pieces=(), held_as=jnp.bfloat16):
    array = jax.random.normal(stream_key, shape, jnp.float32) * deviation
    if len(pieces) > 0:
        array = steps_of(stream_key, shape, pieces, -0.22, 0.18) * array
    return jnp.clip(array, min=-most, max=most).astype(held_as)


def setup_inputs(seed: int = 0) -> dict:
    arg_keys = jax.random.split(jax.random.key(seed), 5)
    return {
        "singular_vectors": centred(arg_keys[0], (ROWS, NV), 1.0, 6.0, ((0, 8), (1, 4)), jnp.float32),
        "reflector_vectors": draw_reflector_vectors(jax.random.fold_in(arg_keys[4], 71), 0),
        "reflector_factors": draw_reflector_factors(jax.random.fold_in(arg_keys[4], 71), 0),
        "sweep_bounds": draw_sweep_bounds(jax.random.fold_in(arg_keys[4], 71), 0),
    }


exact_mode = lax.Precision.HIGHEST

def apply_block(row_block, vectors, factor):
    inner_part = jnp.dot(vectors.astype(jnp.float32), row_block.astype(jnp.float32), precision=exact_mode, preferred_element_type=jnp.float32)
    inner_part = jnp.dot(factor.astype(jnp.float32), inner_part.astype(jnp.float32), precision=exact_mode, preferred_element_type=jnp.float32)
    return row_block - jnp.dot(vectors.T.astype(jnp.float32), inner_part.astype(jnp.float32), precision=exact_mode, preferred_element_type=jnp.float32)

def keep_same(matrix):
    return matrix

def reference(singular_vectors, reflector_vectors, reflector_factors, sweep_bounds):

    def one_sweep(field_now, sweep_id):
        first_row = sweep_bounds[sweep_id, 0]
        last_row = sweep_bounds[sweep_id, 1]

        def one_block(counter, current):
            block_id = (BLOCKS - 1 - counter).astype(jnp.int32)
            start_row = (block_id * BW).astype(jnp.int32)
            is_live = (start_row >= first_row) & (start_row <= last_row)

            def update(matrix):
                row_block = lax.dynamic_slice_in_dim(matrix, start_row, 2 * BW, 0)
                row_block = apply_block(row_block, reflector_vectors[sweep_id, block_id], reflector_factors[sweep_id, block_id])
                return lax.dynamic_update_slice_in_dim(matrix, row_block, start_row, 0)
            return lax.cond(is_live, update, keep_same, current)
        return (lax.fori_loop(0, BLOCKS, one_block, field_now), None)
    result_field, unused = lax.scan(one_sweep, singular_vectors, jnp.arange(SWEEPS, dtype=jnp.int32))
    return result_field
```

```python
import functools

import jax
import jax.numpy as jnp
from jax import lax
from jax.experimental import pallas as pl
from jax.experimental.pallas import tpu as pltpu
from jax.sharding import PartitionSpec as P

MESH = pl.DeviceIdType.MESH
f32, bf16 = jnp.float32, jnp.bfloat16
WIDTH = 128


def split(value):
    high = value.astype(bf16)
    return high, (value - high.astype(f32)).astype(bf16)


def dot3(a, b):
    (a_high, a_low), (b_high, b_low) = a, b
    dot = functools.partial(jnp.dot, preferred_element_type=f32)
    return dot(a_high, b_high) + (dot(a_high, b_low) + dot(a_low, b_high))


def kernel(
    count, ring, bounds_ref, x_ref, vec_ref, fac_ref, out_ref,
    gathered, outbox, upper_high, upper_low, lower_high, lower_low,
    prev, below, tops, returned, middle,
    shift_send, shift_recv, hop_send, hop_recv, far_send, far_recv,
    first_send, first_recv, up_send, up_recv, down_send, down_recv,
):
    me, slab = lax.axis_index("row"), lax.axis_index("col")
    bw = x_ref.shape[0] // 2
    half = bw // 2
    part = bw // ring
    pieces, width = below.shape[1], below.shape[3]
    first, last = me == 0, me == count - 1

    def block_rows(owner):
        return pl.ds(pl.multiple_of(owner * part, part), part)

    def columns(p):
        return pl.ds(pl.multiple_of(p * width, width), width)

    barrier = pltpu.get_barrier_semaphore()

    @pl.when(jnp.logical_not(first))
    def _():
        pl.semaphore_signal(barrier, inc=1, device_id={"row": me - 1}, device_id_type=MESH)

    @pl.when(jnp.logical_not(last))
    def _():
        pl.semaphore_signal(barrier, inc=1, device_id={"row": me + 1}, device_id_type=MESH)

    for k in range(1, ring):
        pl.semaphore_signal(
            barrier, inc=1, device_id={"col": lax.rem(slab + k, ring)}, device_id_type=MESH
        )

    for s in range(2):
        for b, rows in ((1, outbox.at[s]), (0, gathered.at[s, 0, block_rows(slab)])):
            w, f = vec_ref[s, b], fac_ref[s, b]
            rows[:, :bw] = w[:, :bw] + w[:, bw:]
            rows[:, bw:] = jnp.where(slab * part < half, f[:, :half], f[:, half:])

    @pl.when(first)
    def _():
        for s in range(2):
            gathered[s, 1, block_rows(slab)] = jnp.zeros((part, bw + half), f32)
        prev[...] = jnp.zeros_like(prev)

    @pl.when(last)
    def _():
        for p in range(pieces):
            below[0, p] = x_ref[bw:, p * width:(p + 1) * width]

    peers = jnp.where(me > 0, 1, 0) + jnp.where(me < count - 1, 1, 0) + ring - 1
    pl.semaphore_wait(barrier, peers)

    def shift(s):
        return pltpu.make_async_remote_copy(
            src_ref=outbox.at[s], dst_ref=gathered.at[s, 1, block_rows(slab)],
            send_sem=shift_send.at[s], recv_sem=shift_recv.at[s],
            device_id={"row": me + 1}, device_id_type=MESH,
        )

    def initial(p):
        return pltpu.make_async_remote_copy(
            src_ref=x_ref.at[pl.ds(bw, bw), columns(p)], dst_ref=prev.at[0, p],
            send_sem=first_send.at[p], recv_sem=first_recv.at[p],
            device_id={"row": me + 1}, device_id_type=MESH,
        )

    def hop(way, role, t, owner):
        block = gathered.at[0, role, block_rows(owner)]
        return pltpu.make_async_remote_copy(
            src_ref=block, dst_ref=block,
            send_sem=hop_send.at[way, role, t], recv_sem=hop_recv.at[way, role, t],
            device_id={"col": slab + (1 - 2 * way)}, device_id_type=MESH,
        )

    def sends(way, t):
        if way == 0:
            return (slab - t >= 0) & (slab + 1 < ring)
        return (slab + t < ring) & (slab >= 1)

    def gets(way, t):
        return slab - 1 - t >= 0 if way == 0 else slab + 1 + t < ring

    def send_hops(role, t):
        for way in range(2):
            @pl.when(sends(way, t))
            def _():
                hop(way, role, t, slab - (1 - 2 * way) * t).start()

    def get_hops(role, t):
        for way in range(2):
            @pl.when(gets(way, t))
            def _():
                hop(way, role, t, slab - (1 - 2 * way) * (t + 1)).wait_recv()

    def far(role, k, owner):
        block = gathered.at[1, role, block_rows(owner)]
        return pltpu.make_async_remote_copy(
            src_ref=block, dst_ref=block,
            send_sem=far_send.at[role, k], recv_sem=far_recv.at[role, k],
            device_id={"col": lax.rem(slab + k, ring)}, device_id_type=MESH,
        )

    send_hops(0, 0)

    @pl.when(jnp.logical_not(last))
    def _():
        shift(0).start()
        shift(1).start()
        for p in range(pieces):
            initial(p).start()

    @pl.when(jnp.logical_not(first))
    def _():
        shift(0).wait_recv()

    send_hops(1, 0)
    for t in range(ring - 1):
        for role in range(2):
            get_hops(role, t)
            if t + 1 < ring - 1:
                send_hops(role, t + 1)

    @pl.when(jnp.logical_not(first))
    def _():
        shift(1).wait_recv()

    for role in range(2):
        for k in range(1, ring):
            far(role, k, slab).start()

    def build(s):
        row = lax.broadcasted_iota(jnp.int32, (bw, bw), 0)
        col = lax.broadcasted_iota(jnp.int32, (bw, bw), 1)
        row2 = lax.broadcasted_iota(jnp.int32, (2 * bw, 2 * bw), 0)
        col2 = lax.broadcasted_iota(jnp.int32, (2 * bw, 2 * bw), 1)
        unit = jnp.where(row2 == col2, 1.0, 0.0).astype(f32)

        def whole(role):
            start = (me * 2 - role) * bw
            live = (start >= bounds_ref[s, 0]) & (start <= bounds_ref[s, 1])
            packed = gathered[s, role, :, :bw]
            factor = gathered[s, role, :, bw:] * jnp.where(live, 1.0, 0.0).astype(f32)
            w = jnp.concatenate(
                [jnp.where(col >= row, packed, 0.0), jnp.where(col < row, packed, 0.0)], axis=1
            )
            w_high, w_low = split(w)
            head, tail = (w_high[:half], w_low[:half]), (w_high[half:], w_low[half:])
            g_tail = dot3(split(factor[half:]), tail)
            u = dot3(head, tuple(value.T for value in tail))
            g_head = dot3(split(factor[:half]), split(w[:half] - dot3(split(u), split(g_tail))))
            g = jnp.concatenate([g_head, g_tail], axis=0)
            return unit - dot3((w_high.T, w_low.T), split(g))

        q1 = whole(0)
        lower_high[s], lower_low[s] = split(q1[bw:])
        q0 = whole(1)
        mixed = dot3(split(q0[:, bw:]), split(q1[:bw]))
        upper_high[s, :, :bw], upper_low[s, :, :bw] = split(q0[:, :bw])
        upper_high[s, :, bw:], upper_low[s, :, bw:] = split(mixed)

    def up(s, p):
        return pltpu.make_async_remote_copy(
            src_ref=tops.at[s, p], dst_ref=below.at[s, p],
            send_sem=up_send.at[s, p], recv_sem=up_recv.at[s, p],
            device_id={"row": me - 1}, device_id_type=MESH,
        )

    def down(p):
        return pltpu.make_async_remote_copy(
            src_ref=returned.at[p], dst_ref=prev.at[1, p],
            send_sem=down_send.at[p], recv_sem=down_recv.at[p],
            device_id={"row": me + 1}, device_id_type=MESH,
        )

    def sweep(s):
        def piece(p, carry):
            @pl.when(jnp.logical_not(first))
            def _():
                (initial(p) if s == 0 else down(p)).wait_recv()

            @pl.when(jnp.logical_not(last))
            def _():
                up(s, p).wait_recv()

            x0 = x_ref[:bw, columns(p)] if s == 0 else middle[p]
            parts = split(jnp.concatenate([prev[s, p], x0, below[s, p]], axis=0))
            tops[s, p] = dot3((upper_high[s, :bw], upper_low[s, :bw]), parts)

            @pl.when(jnp.logical_not(first))
            def _():
                up(s, p).start()

            ended = dot3((lower_high[s], lower_low[s]), tuple(value[bw:] for value in parts))
            if s == 0:
                returned[p] = ended

                @pl.when(jnp.logical_not(last))
                def _():
                    down(p).start()

                @pl.when(last)
                def _():
                    below[1, p] = returned[p]
            else:
                out_ref[bw:, columns(p)] = ended

            kept = dot3((upper_high[s, bw:], upper_low[s, bw:]), parts)
            if s == 0:
                middle[p] = kept
            else:
                out_ref[:bw, columns(p)] = kept

            return carry

        lax.fori_loop(0, pieces, piece, 0)

    build(0)
    sweep(0)
    for role in range(2):
        for k in range(1, ring):
            far(role, k, lax.rem(slab + ring - k, ring)).wait_recv()
    build(1)
    sweep(1)

    for role in range(2):
        for t in range(ring - 1):
            for way in range(2):
                @pl.when(sends(way, t))
                def _():
                    hop(way, role, t, slab).wait_send()

        for k in range(1, ring):
            far(role, k, slab).wait_send()

    @pl.when(jnp.logical_not(last))
    def _():
        shift(0).wait_send()
        shift(1).wait_send()

    def finish(p, carry):
        @pl.when(jnp.logical_not(first))
        def _():
            up(0, p).wait_send()
            up(1, p).wait_send()

        @pl.when(jnp.logical_not(last))
        def _():
            initial(p).wait_send()
            down(p).wait_send()

        return carry

    lax.fori_loop(0, pieces, finish, 0)


def per_device(singular_vectors, reflector_vectors, reflector_factors, sweep_bounds):
    count, ring = lax.axis_size("row"), lax.axis_size("col")
    rows, cols = singular_vectors.shape
    sweeps, blocks, _, span = reflector_vectors.shape
    bw = span // 2
    assert sweeps == 2 and blocks == 2 and rows == span and cols % WIDTH == 0
    pieces = cols // WIDTH
    vmem, dma = pltpu.VMEM, pltpu.SemaphoreType.DMA
    return pl.pallas_call(
        functools.partial(kernel, count, ring),
        out_shape=jax.ShapeDtypeStruct((rows, cols), f32),
        in_specs=[pl.BlockSpec(memory_space=pltpu.SMEM)] + [pl.BlockSpec(memory_space=vmem)] * 3,
        out_specs=pl.BlockSpec(memory_space=vmem),
        scratch_shapes=[
            vmem((2, 2, bw, bw + bw // 2), f32),
            vmem((2, bw // ring, bw + bw // 2), f32),
            vmem((2, span, 3 * bw), bf16), vmem((2, span, 3 * bw), bf16),
            vmem((2, bw, span), bf16), vmem((2, bw, span), bf16),
            vmem((2, pieces, bw, WIDTH), f32),
            vmem((2, pieces, bw, WIDTH), f32),
            vmem((2, pieces, bw, WIDTH), f32),
            vmem((pieces, bw, WIDTH), f32),
            vmem((pieces, bw, WIDTH), f32),
            dma((2,)), dma((2,)), dma((2, 2, ring)), dma((2, 2, ring)),
            dma((2, ring)), dma((2, ring)), dma((pieces,)), dma((pieces,)),
            dma((2, pieces)), dma((2, pieces)), dma((pieces,)), dma((pieces,)),
        ],
        compiler_params=pltpu.CompilerParams(
            collective_id=0, has_side_effects=True, vmem_limit_bytes=56 * 2**20
        ),
    )(sweep_bounds, singular_vectors, reflector_vectors, reflector_factors)


def solution(mesh):
    placed = (P("row", "col"), P(None, "row", "col", None), P(None, "row", "col", None), P())
    return jax.shard_map(
        per_device, mesh=mesh, in_specs=placed, out_specs=P("row", "col"), check_vma=False
    )
```

```python
import functools

import jax
import jax.numpy as jnp
from jax import lax
from jax.experimental import pallas as pl
from jax.experimental.pallas import tpu as pltpu
from jax.sharding import PartitionSpec as P

MESH = pl.DeviceIdType.MESH
f32, bf16 = jnp.float32, jnp.bfloat16
WIDTH = 128


def split(value):
    high = value.astype(bf16)
    return high, (value - high.astype(f32)).astype(bf16)


def dot3(a, b):
    (a_high, a_low), (b_high, b_low) = a, b
    dot = functools.partial(jnp.dot, preferred_element_type=f32)
    return dot(a_high, b_high) + (dot(a_high, b_low) + dot(a_low, b_high))


LOW0, UP0, LOW1, UP1, EXTRA = range(5)
LAG = 2


def kernel(
    count, ring, bounds_ref, x_ref, vec_ref, fac_ref, out_ref,
    gathered, outbox, upper_high, upper_low, lower_high, lower_low, extra_high, extra_low,
    window, below, tops,
    shift_send, shift_recv, hop_send, hop_recv,
    first_send, first_recv, up_send, up_recv,
):
    me, slab = lax.axis_index("row"), lax.axis_index("col")
    bw = x_ref.shape[0] // 2
    half = bw // 2
    part = bw // ring
    pieces, width = below.shape[1], below.shape[3]
    first, last = me == 0, me == count - 1
    inner = jnp.logical_not(first)

    def block_rows(owner):
        return pl.ds(pl.multiple_of(owner * part, part), part)

    def columns(p):
        return pl.ds(pl.multiple_of(p * width, width), width)

    barrier = pltpu.get_barrier_semaphore()

    @pl.when(inner)
    def _():
        pl.semaphore_signal(barrier, inc=1, device_id={"row": me - 1}, device_id_type=MESH)

    @pl.when(jnp.logical_not(last))
    def _():
        pl.semaphore_signal(barrier, inc=1, device_id={"row": me + 1}, device_id_type=MESH)

    for way in range(2):
        @pl.when(slab + 1 < ring if way == 0 else slab >= 1)
        def _():
            pl.semaphore_signal(
                barrier, inc=1, device_id={"col": slab + (1 - 2 * way)}, device_id_type=MESH
            )

    def stage(rows, s, b):
        w, f = vec_ref[s, b], fac_ref[s, b]
        rows[:, :bw] = w[:, :bw] + w[:, bw:]
        rows[:, bw:] = jnp.where(slab * part < half, f[:, :half], f[:, half:])

    moved = ((LOW0, 0, 1), (UP0, 0, 0), (UP1, 1, 1))
    for k, (slot, s, b) in enumerate(moved):
        stage(outbox.at[k], s, b)
    stage(gathered.at[LOW1, block_rows(slab)], 1, 0)

    @pl.when(last)
    def _():
        stage(gathered.at[EXTRA, block_rows(slab)], 0, 0)

    @pl.when(first)
    def _():
        gathered[UP1] = jnp.zeros((bw, bw + half), f32)
        window[0] = jnp.zeros_like(window[0])

    def greeted(there):
        return jnp.where(there, 1, 0)

    pl.semaphore_wait(
        barrier,
        greeted(me > 0) + greeted(me < count - 1) + greeted(slab > 0) + greeted(slab < ring - 1),
    )

    def shift(k):
        return pltpu.make_async_remote_copy(
            src_ref=outbox.at[k], dst_ref=gathered.at[moved[k][0], block_rows(slab)],
            send_sem=shift_send.at[k], recv_sem=shift_recv.at[k],
            device_id={"row": me + 1}, device_id_type=MESH,
        )

    def initial(h, p):
        return pltpu.make_async_remote_copy(
            src_ref=x_ref.at[pl.ds(h * bw, bw), columns(p)], dst_ref=window.at[h, p],
            send_sem=first_send.at[h, p], recv_sem=first_recv.at[h, p],
            device_id={"row": me + 1}, device_id_type=MESH,
        )

    def hop(way, slot, t, owner):
        block = gathered.at[slot, block_rows(owner)]
        return pltpu.make_async_remote_copy(
            src_ref=block, dst_ref=block,
            send_sem=hop_send.at[way, slot, t], recv_sem=hop_recv.at[way, slot, t],
            device_id={"col": slab + (1 - 2 * way)}, device_id_type=MESH,
        )

    def sends(way, t):
        if way == 0:
            return (slab - t >= 0) & (slab + 1 < ring)
        return (slab + t < ring) & (slab >= 1)

    def gets(way, t):
        return slab - 1 - t >= 0 if way == 0 else slab + 1 + t < ring

    def send_hops(slot, t, when):
        for way in range(2):
            @pl.when(when & (t < ring - 1) & sends(way, t))
            def _():
                hop(way, slot, t, slab - (1 - 2 * way) * t).start()

    def get_hops(slot, t, when):
        for way in range(2):
            @pl.when(when & gets(way, t))
            def _():
                hop(way, slot, t, slab - (1 - 2 * way) * (t + 1)).wait_recv()

    send_hops(EXTRA, 0, last)

    @pl.when(jnp.logical_not(last))
    def _():
        for k in range(len(moved)):
            shift(k).start()
        for p in range(pieces):
            for h in range(2):
                initial(h, p).start()

    for k, slot in enumerate((LOW0, UP0)):
        @pl.when(inner)
        def _():
            shift(k).wait_recv()

        send_hops(slot, 0, inner)

    for t in range(ring - 1):
        for slot in (EXTRA, LOW0, UP0):
            if t == ring - 2 and slot == UP0:
                break
            when = last if slot == EXTRA else inner
            get_hops(slot, t, when)
            send_hops(slot, t + 1, when)

    send_hops(LOW1, 0, slab >= 0)

    @pl.when(inner)
    def _():
        shift(2).wait_recv()

    send_hops(UP1, 0, inner)

    def whole(slot, s, block):
        row = lax.broadcasted_iota(jnp.int32, (bw, bw), 0)
        col = lax.broadcasted_iota(jnp.int32, (bw, bw), 1)
        row2 = lax.broadcasted_iota(jnp.int32, (2 * bw, 2 * bw), 0)
        col2 = lax.broadcasted_iota(jnp.int32, (2 * bw, 2 * bw), 1)
        unit = jnp.where(row2 == col2, 1.0, 0.0).astype(f32)
        start = block * bw
        live = (start >= bounds_ref[s, 0]) & (start <= bounds_ref[s, 1])
        packed = gathered[slot, :, :bw]
        factor = gathered[slot, :, bw:] * jnp.where(live, 1.0, 0.0).astype(f32)
        w = jnp.concatenate(
            [jnp.where(col >= row, packed, 0.0), jnp.where(col < row, packed, 0.0)], axis=1
        )
        w_high, w_low = split(w)
        head, tail = (w_high[:half], w_low[:half]), (w_high[half:], w_low[half:])
        g_tail = dot3(split(factor[half:]), tail)
        u = dot3(head, tuple(value.T for value in tail))
        g_head = dot3(split(factor[:half]), split(w[:half] - dot3(split(u), split(g_tail))))
        g = jnp.concatenate([g_head, g_tail], axis=0)
        return unit - dot3((w_high.T, w_low.T), split(g))

    def build_low(s):
        lower_high[s], lower_low[s] = split(whole(2 * s, s, 2 * me - 1 + s))

    def build_up(s):
        q = whole(2 * s + 1, s, 2 * me - 2 + s)
        mixed = dot3(split(q[:, bw:]), (lower_high[s, :bw], lower_low[s, :bw]))
        upper_high[s, :, :bw], upper_low[s, :, :bw] = split(q[:, :bw])
        upper_high[s, :, bw:], upper_low[s, :, bw:] = split(mixed)

    @pl.when(last)
    def _():
        extra_high[...], extra_low[...] = split(whole(EXTRA, 0, 2 * me))

        def own(p, carry):
            both = dot3((extra_high[...], extra_low[...]), split(x_ref[:, columns(p)]))
            below[0, p], below[1, p] = both[:bw], both[bw:]
            return carry

        lax.fori_loop(0, pieces, own, 0)

    @pl.when(inner)
    def _():
        build_low(0)

    get_hops(UP0, ring - 2, inner)

    @pl.when(inner)
    def _():
        build_up(0)

    def up(s, p):
        return pltpu.make_async_remote_copy(
            src_ref=tops.at[s, p], dst_ref=below.at[s, p],
            send_sem=up_send.at[s, p], recv_sem=up_recv.at[s, p],
            device_id={"row": me - 1}, device_id_type=MESH,
        )

    def second(q, carry):
        t, slot = q // 2, LOW1 + q % 2
        when = inner | (slot == LOW1)
        get_hops(slot, t, when)
        send_hops(slot, t + 1, when)
        return carry

    def apply(s, p):
        parts = split(jnp.concatenate([window[0, p], window[1, p], below[s, p]], axis=0))

        @pl.when(inner)
        def _():
            tops[s, p] = dot3((upper_high[s, :bw], upper_low[s, :bw]), parts)
            up(s, p).start()

        ended = dot3((lower_high[s, bw:], lower_low[s, bw:]), tuple(value[bw:] for value in parts))
        kept = dot3((upper_high[s, bw:], upper_low[s, bw:]), parts)
        if s == 0:
            window[0, p], window[1, p] = kept, ended
        else:
            out_ref[:bw, columns(p)], out_ref[bw:, columns(p)] = kept, ended

    steps = 2 * (ring - 1)

    def first_sweep(p, carry):
        @pl.when((p >= LAG) & (p - LAG < steps))
        def _():
            second(p - LAG, 0)

        @pl.when(jnp.logical_not(last))
        def _():
            up(0, p).wait_recv()

        @pl.when(first)
        def _():
            window[1, p] = below[0, p]

        @pl.when(inner)
        def _():
            for h in range(2):
                initial(h, p).wait_recv()
            apply(0, p)

        return carry

    def second_sweep(p, carry):
        @pl.when(jnp.logical_not(last))
        def _():
            up(1, p).wait_recv()

        apply(1, p)
        return carry

    lax.fori_loop(0, pieces, first_sweep, 0)
    if steps > pieces - LAG:
        lax.fori_loop(max(pieces - LAG, 0), steps, second, 0)
    build_low(1)
    build_up(1)
    lax.fori_loop(0, pieces, second_sweep, 0)

    for slot, when in ((LOW0, inner), (UP0, inner), (LOW1, slab >= 0), (UP1, inner), (EXTRA, last)):
        for t in range(ring - 1):
            for way in range(2):
                @pl.when(when & sends(way, t))
                def _():
                    hop(way, slot, t, slab).wait_send()

    @pl.when(jnp.logical_not(last))
    def _():
        for k in range(len(moved)):
            shift(k).wait_send()

    def finish(p, carry):
        @pl.when(inner)
        def _():
            up(0, p).wait_send()
            up(1, p).wait_send()

        @pl.when(jnp.logical_not(last))
        def _():
            initial(0, p).wait_send()
            initial(1, p).wait_send()

        return carry

    lax.fori_loop(0, pieces, finish, 0)


def per_device(singular_vectors, reflector_vectors, reflector_factors, sweep_bounds):
    count, ring = lax.axis_size("row"), lax.axis_size("col")
    rows, cols = singular_vectors.shape
    sweeps, blocks, _, span = reflector_vectors.shape
    bw = span // 2
    assert sweeps == 2 and blocks == 2 and rows == span and cols % WIDTH == 0
    pieces = cols // WIDTH
    vmem, dma = pltpu.VMEM, pltpu.SemaphoreType.DMA
    return pl.pallas_call(
        functools.partial(kernel, count, ring),
        out_shape=jax.ShapeDtypeStruct((rows, cols), f32),
        in_specs=[pl.BlockSpec(memory_space=pltpu.SMEM)] + [pl.BlockSpec(memory_space=vmem)] * 3,
        out_specs=pl.BlockSpec(memory_space=vmem),
        scratch_shapes=[
            vmem((5, bw, bw + bw // 2), f32),
            vmem((3, bw // ring, bw + bw // 2), f32),
            vmem((2, span, 3 * bw), bf16), vmem((2, span, 3 * bw), bf16),
            vmem((2, span, span), bf16), vmem((2, span, span), bf16),
            vmem((span, span), bf16), vmem((span, span), bf16),
            vmem((2, pieces, bw, WIDTH), f32),
            vmem((2, pieces, bw, WIDTH), f32),
            vmem((2, pieces, bw, WIDTH), f32),
            dma((3,)), dma((3,)), dma((2, 5, ring)), dma((2, 5, ring)),
            dma((2, pieces)), dma((2, pieces)), dma((2, pieces)), dma((2, pieces)),
        ],
        compiler_params=pltpu.CompilerParams(
            collective_id=0, has_side_effects=True, vmem_limit_bytes=56 * 2**20
        ),
    )(sweep_bounds, singular_vectors, reflector_vectors, reflector_factors)


def solution(mesh):
    placed = (P("row", "col"), P(None, "row", "col", None), P(None, "row", "col", None), P())
    return jax.shard_map(
        per_device, mesh=mesh, in_specs=placed, out_specs=P("row", "col"), check_vma=False
    )
```

```python
import functools

import jax
import jax.numpy as jnp
from jax import lax
from jax.experimental import pallas as pl
from jax.experimental.pallas import tpu as pltpu
from jax.sharding import PartitionSpec as P

MESH = pl.DeviceIdType.MESH
f32, bf16 = jnp.float32, jnp.bfloat16
WIDTH = 128


def split(value):
    high = value.astype(bf16)
    return high, (value - high.astype(f32)).astype(bf16)


def dot3(a, b):
    (a_high, a_low), (b_high, b_low) = a, b
    dot = functools.partial(jnp.dot, preferred_element_type=f32)
    return dot(a_high, b_high) + (dot(a_high, b_low) + dot(a_low, b_high))


LOW0, UP0, LOW1, UP1, EXTRA = range(5)


def kernel(
    count, ring, bounds_ref, x_ref, vec_ref, fac_ref, out_ref,
    gathered, outbox, upper_high, upper_low, lower_high, lower_low, extra_high, extra_low,
    cross, crossed, cross_high, cross_low,
    window, below, tops, partner, nearby, local,
    shift_send, shift_recv, hop_send, hop_recv, far_send, far_recv, cross_send, cross_recv,
    first_send, first_recv, up_send, up_recv, over_send, over_recv, near_send, near_recv,
):
    me, slab = lax.axis_index("row"), lax.axis_index("col")
    bw = x_ref.shape[0] // 2
    half = bw // 2
    part = bw // ring
    pairs, width = below.shape[1], WIDTH
    pieces = 2 * pairs
    first, last = me == 0, me == count - 1
    inner = jnp.logical_not(first)
    odd = lax.rem(me, 2) == 1
    even = jnp.logical_not(odd)

    def block_rows(owner):
        return pl.ds(pl.multiple_of(owner * part, part), part)

    def columns(p):
        return pl.ds(pl.multiple_of(p * width, width), width)

    def lanes(p):
        return columns(lax.rem(p, 2))

    def broad(q):
        return pl.ds(pl.multiple_of(q * 2 * width, 2 * width), 2 * width)

    barrier = pltpu.get_barrier_semaphore()

    @pl.when(inner)
    def _():
        pl.semaphore_signal(barrier, inc=1, device_id={"row": me - 1}, device_id_type=MESH)

    @pl.when(jnp.logical_not(last))
    def _():
        pl.semaphore_signal(barrier, inc=1, device_id={"row": me + 1}, device_id_type=MESH)

    @pl.when(odd & (me > 1))
    def _():
        pl.semaphore_signal(barrier, inc=1, device_id={"row": me - 2}, device_id_type=MESH)

    @pl.when(odd & (me + 2 < count))
    def _():
        pl.semaphore_signal(barrier, inc=1, device_id={"row": me + 2}, device_id_type=MESH)

    for k in range(1, ring):
        pl.semaphore_signal(
            barrier, inc=1, device_id={"col": lax.rem(slab + k, ring)}, device_id_type=MESH
        )

    def stage(rows, s, b):
        w, f = vec_ref[s, b], fac_ref[s, b]
        rows[:, :bw] = w[:, :bw] + w[:, bw:]
        rows[:, bw:] = jnp.where(slab * part < half, f[:, :half], f[:, half:])

    moved = ((LOW0, 0, 1), (UP0, 0, 0), (UP1, 1, 1))
    for k, (slot, s, b) in enumerate(moved):
        stage(outbox.at[k], s, b)
    stage(gathered.at[LOW1, block_rows(slab)], 1, 0)

    @pl.when(last)
    def _():
        stage(gathered.at[EXTRA, block_rows(slab)], 0, 0)

    @pl.when(first)
    def _():
        gathered[UP1] = jnp.zeros((bw, bw + half), f32)
        window[0] = jnp.zeros_like(window[0])

    def greeted(there):
        return jnp.where(there, 1, 0)

    pl.semaphore_wait(
        barrier,
        greeted(me > 0) + greeted(me < count - 1) + ring - 1
        + greeted(odd & (me > 1)) + greeted(odd & (me + 2 < count)),
    )

    def shift(k):
        return pltpu.make_async_remote_copy(
            src_ref=outbox.at[k], dst_ref=gathered.at[moved[k][0], block_rows(slab)],
            send_sem=shift_send.at[k], recv_sem=shift_recv.at[k],
            device_id={"row": me + 1}, device_id_type=MESH,
        )

    def initial(h, p):
        return pltpu.make_async_remote_copy(
            src_ref=x_ref.at[pl.ds(h * bw, bw), columns(p)], dst_ref=window.at[h, p // 2, :, lanes(p)],
            send_sem=first_send.at[h, p], recv_sem=first_recv.at[h, p],
            device_id={"row": me + 1}, device_id_type=MESH,
        )

    def hop(way, slot, t, owner):
        block = gathered.at[slot, block_rows(owner)]
        return pltpu.make_async_remote_copy(
            src_ref=block, dst_ref=block,
            send_sem=hop_send.at[way, slot, t], recv_sem=hop_recv.at[way, slot, t],
            device_id={"col": slab + (1 - 2 * way)}, device_id_type=MESH,
        )

    def sends(way, t):
        if way == 0:
            return (slab - t >= 0) & (slab + 1 < ring)
        return (slab + t < ring) & (slab >= 1)

    def gets(way, t):
        return slab - 1 - t >= 0 if way == 0 else slab + 1 + t < ring

    def send_hops(slot, t, when):
        for way in range(2):
            @pl.when(when & (t < ring - 1) & sends(way, t))
            def _():
                hop(way, slot, t, slab - (1 - 2 * way) * t).start()

    def get_hops(slot, t, when):
        for way in range(2):
            @pl.when(when & gets(way, t))
            def _():
                hop(way, slot, t, slab - (1 - 2 * way) * (t + 1)).wait_recv()

    send_hops(EXTRA, 0, last)

    @pl.when(jnp.logical_not(last))
    def _():
        for k in range(len(moved)):
            shift(k).start()
        for p in range(pieces):
            for h in range(2):
                initial(h, p).start()

    for k, slot in enumerate((LOW0, UP0)):
        @pl.when(inner)
        def _():
            shift(k).wait_recv()

        send_hops(slot, 0, inner)

    for t in range(ring - 1):
        for slot in (EXTRA, LOW0, UP0):
            if t == ring - 2 and slot == UP0:
                break
            when = last if slot == EXTRA else inner
            get_hops(slot, t, when)
            send_hops(slot, t + 1, when)

    def far(slot, k, owner):
        block = gathered.at[slot, block_rows(owner)]
        return pltpu.make_async_remote_copy(
            src_ref=block, dst_ref=block,
            send_sem=far_send.at[slot - LOW1, k], recv_sem=far_recv.at[slot - LOW1, k],
            device_id={"col": lax.rem(slab + k, ring)}, device_id_type=MESH,
        )

    for k in range(1, ring):
        far(LOW1, k, slab).start()

    @pl.when(inner)
    def _():
        shift(2).wait_recv()
        for k in range(1, ring):
            far(UP1, k, slab).start()

    def whole(slot, s, block):
        row = lax.broadcasted_iota(jnp.int32, (bw, bw), 0)
        col = lax.broadcasted_iota(jnp.int32, (bw, bw), 1)
        row2 = lax.broadcasted_iota(jnp.int32, (2 * bw, 2 * bw), 0)
        col2 = lax.broadcasted_iota(jnp.int32, (2 * bw, 2 * bw), 1)
        unit = jnp.where(row2 == col2, 1.0, 0.0).astype(f32)
        start = block * bw
        live = (start >= bounds_ref[s, 0]) & (start <= bounds_ref[s, 1])
        packed = gathered[slot, :, :bw]
        factor = gathered[slot, :, bw:] * jnp.where(live, 1.0, 0.0).astype(f32)
        w = jnp.concatenate(
            [jnp.where(col >= row, packed, 0.0), jnp.where(col < row, packed, 0.0)], axis=1
        )
        w_high, w_low = split(w)
        head, tail = (w_high[:half], w_low[:half]), (w_high[half:], w_low[half:])
        g_tail = dot3(split(factor[half:]), tail)
        u = dot3(head, tuple(value.T for value in tail))
        g_head = dot3(split(factor[:half]), split(w[:half] - dot3(split(u), split(g_tail))))
        g = jnp.concatenate([g_head, g_tail], axis=0)
        return unit - dot3((w_high.T, w_low.T), split(g))

    def build_low(s):
        lower_high[s], lower_low[s] = split(whole(2 * s, s, 2 * me - 1 + s))

    def build_up(s):
        q = whole(2 * s + 1, s, 2 * me - 2 + s)
        mixed = dot3(split(q[:, bw:]), (lower_high[s, :bw], lower_low[s, :bw]))
        upper_high[s, :, :bw], upper_low[s, :, :bw] = split(q[:, :bw])
        upper_high[s, :, bw:], upper_low[s, :, bw:] = split(mixed)

        @pl.when(even & inner)
        def _():
            cross[s] = mixed[:bw, bw:]
            across(s).start()

    def across(s):
        return pltpu.make_async_remote_copy(
            src_ref=cross.at[s], dst_ref=crossed.at[s],
            send_sem=cross_send.at[s], recv_sem=cross_recv.at[s],
            device_id={"row": me + 1}, device_id_type=MESH,
        )

    def get_across(s):
        @pl.when(odd & (me > 1))
        def _():
            across(s).wait_recv()
            cross_high[s], cross_low[s] = split(crossed[s])

    @pl.when(last)
    def _():
        extra_high[...], extra_low[...] = split(whole(EXTRA, 0, 2 * me))

        def own(p, carry):
            both = dot3((extra_high[...], extra_low[...]), split(x_ref[:, broad(p)]))
            below[0, p], below[1, p] = both[:bw], both[bw:]
            return carry

        lax.fori_loop(0, pairs, own, 0)

    @pl.when(inner)
    def _():
        build_low(0)

    get_hops(UP0, ring - 2, inner)

    @pl.when(inner)
    def _():
        build_up(0)

    def up(s, p):
        block = (s, p // 2, slice(None), lanes(p))
        return pltpu.make_async_remote_copy(
            src_ref=tops.at[block], dst_ref=below.at[block],
            send_sem=up_send.at[s, p], recv_sem=up_recv.at[s, p],
            device_id={"row": me - 2}, device_id_type=MESH,
        )

    def over(s, p):
        block = (s, p // 2, slice(None), lanes(p))
        return pltpu.make_async_remote_copy(
            src_ref=partner.at[block], dst_ref=below.at[block],
            send_sem=over_send.at[s, p], recv_sem=over_recv.at[s, p],
            device_id={"row": me - 1}, device_id_type=MESH,
        )

    def near(s, q):
        return pltpu.make_async_remote_copy(
            src_ref=partner.at[s, q], dst_ref=nearby.at[s, q],
            send_sem=near_send.at[s, q], recv_sem=near_recv.at[s, q],
            device_id={"row": me + 1}, device_id_type=MESH,
        )

    def get_initial(q):
        for h in range(2):
            for i in range(2):
                initial(h, 2 * q + i).wait_recv()

    def share(s, q):
        parts = split(jnp.concatenate([window[0, q], window[1, q]], axis=0))
        return dot3((upper_high[s, :bw, :2 * bw], upper_low[s, :bw, :2 * bw]), parts)

    def settle(s, q):
        parts = split(jnp.concatenate([window[0, q], window[1, q], below[s, q]], axis=0))
        kept = dot3((upper_high[s, bw:], upper_low[s, bw:]), parts)
        ended = dot3((lower_high[s, bw:], lower_low[s, bw:]), tuple(value[bw:] for value in parts))
        if s == 0:
            window[0, q], window[1, q] = kept, ended
        else:
            out_ref[:bw, broad(q)], out_ref[bw:, broad(q)] = kept, ended

    def odd_sweep(s):
        def pair(q, carry):
            if s == 0:
                get_initial(q)
            local[...] = share(s, q)

            @pl.when(me > 1)
            def _():
                near(s, q).wait_recv()

            for i in range(2):
                p = 2 * q + i
                half_lanes = slice(i * width, (i + 1) * width)

                @pl.when(jnp.logical_not(last))
                def _():
                    up(s, p).wait_recv()

                step = (upper_high[s, :bw, 2 * bw:], upper_low[s, :bw, 2 * bw:])
                mine = local[:, half_lanes] + dot3(step, split(below[s, q, :, half_lanes]))
                partner[s, q, :, half_lanes] = mine

                @pl.when(me > 1)
                def _():
                    step = (cross_high[s], cross_low[s])
                    tops[s, q, :, half_lanes] = nearby[s, q, :, half_lanes] + dot3(step, split(mine))
                    up(s, p).start()

                over(s, p).start()

            settle(s, q)
            return carry

        lax.fori_loop(0, pairs, pair, 0)

    def even_sweep(s):
        def pair(q, carry):
            @pl.when((q < pairs) & inner)
            def _():
                if s == 0:
                    get_initial(q)
                partner[s, q] = share(s, q)
                near(s, q).start()

            @pl.when(q >= 1)
            def _():
                over(s, 2 * q - 2).wait_recv()
                over(s, 2 * q - 1).wait_recv()
                if s == 1:
                    settle(s, q - 1)

            if s == 0:
                @pl.when((q >= 1) & inner)
                def _():
                    settle(s, q - 1)

                @pl.when((q >= 1) & first)
                def _():
                    window[1, q - 1] = below[0, q - 1]

            return carry

        lax.fori_loop(0, pairs + 1, pair, 0)

    def sweep(s):
        get_across(s)

        @pl.when(odd)
        def _():
            odd_sweep(s)

        @pl.when(even)
        def _():
            even_sweep(s)

    sweep(0)
    for k in range(1, ring):
        far(LOW1, k, lax.rem(slab + ring - k, ring)).wait_recv()

    @pl.when(inner)
    def _():
        for k in range(1, ring):
            far(UP1, k, lax.rem(slab + ring - k, ring)).wait_recv()

    build_low(1)
    build_up(1)
    sweep(1)

    for slot, when in ((LOW0, inner), (UP0, inner), (EXTRA, last)):
        for t in range(ring - 1):
            for way in range(2):
                @pl.when(when & sends(way, t))
                def _():
                    hop(way, slot, t, slab).wait_send()

    for k in range(1, ring):
        far(LOW1, k, slab).wait_send()

    @pl.when(inner)
    def _():
        for k in range(1, ring):
            far(UP1, k, slab).wait_send()

    @pl.when(jnp.logical_not(last))
    def _():
        for k in range(len(moved)):
            shift(k).wait_send()

    @pl.when(even & inner)
    def _():
        across(0).wait_send()
        across(1).wait_send()

    def finish(p, carry):
        for s in range(2):
            @pl.when(odd & (me > 1))
            def _():
                up(s, p).wait_send()

            @pl.when(odd)
            def _():
                over(s, p).wait_send()

            @pl.when(even & inner & (p < pairs))
            def _():
                near(s, p).wait_send()

        @pl.when(jnp.logical_not(last))
        def _():
            initial(0, p).wait_send()
            initial(1, p).wait_send()

        return carry

    lax.fori_loop(0, pieces, finish, 0)


def per_device(singular_vectors, reflector_vectors, reflector_factors, sweep_bounds):
    count, ring = lax.axis_size("row"), lax.axis_size("col")
    rows, cols = singular_vectors.shape
    sweeps, blocks, _, span = reflector_vectors.shape
    bw = span // 2
    assert sweeps == 2 and blocks == 2 and rows == span and cols % (2 * WIDTH) == 0
    assert count % 2 == 0
    pairs = cols // (2 * WIDTH)
    vmem, dma = pltpu.VMEM, pltpu.SemaphoreType.DMA
    return pl.pallas_call(
        functools.partial(kernel, count, ring),
        out_shape=jax.ShapeDtypeStruct((rows, cols), f32),
        in_specs=[pl.BlockSpec(memory_space=pltpu.SMEM)] + [pl.BlockSpec(memory_space=vmem)] * 3,
        out_specs=pl.BlockSpec(memory_space=vmem),
        scratch_shapes=[
            vmem((5, bw, bw + bw // 2), f32),
            vmem((3, bw // ring, bw + bw // 2), f32),
            vmem((2, span, 3 * bw), bf16), vmem((2, span, 3 * bw), bf16),
            vmem((2, span, span), bf16), vmem((2, span, span), bf16),
            vmem((span, span), bf16), vmem((span, span), bf16),
            vmem((2, bw, bw), f32), vmem((2, bw, bw), f32),
            vmem((2, bw, bw), bf16), vmem((2, bw, bw), bf16),
            vmem((2, pairs, bw, 2 * WIDTH), f32),
            vmem((2, pairs, bw, 2 * WIDTH), f32),
            vmem((2, pairs, bw, 2 * WIDTH), f32),
            vmem((2, pairs, bw, 2 * WIDTH), f32),
            vmem((2, pairs, bw, 2 * WIDTH), f32),
            vmem((bw, 2 * WIDTH), f32),
            dma((3,)), dma((3,)), dma((2, 5, ring)), dma((2, 5, ring)),
            dma((2, ring)), dma((2, ring)), dma((2,)), dma((2,)),
            dma((2, 2 * pairs)), dma((2, 2 * pairs)), dma((2, 2 * pairs)), dma((2, 2 * pairs)),
            dma((2, 2 * pairs)), dma((2, 2 * pairs)), dma((2, pairs)), dma((2, pairs)),
        ],
        compiler_params=pltpu.CompilerParams(
            collective_id=0, has_side_effects=True, vmem_limit_bytes=56 * 2**20
        ),
    )(sweep_bounds, singular_vectors, reflector_vectors, reflector_factors)


def solution(mesh):
    placed = (P("row", "col"), P(None, "row", "col", None), P(None, "row", "col", None), P())
    return jax.shard_map(
        per_device, mesh=mesh, in_specs=placed, out_specs=P("row", "col"), check_vma=False
    )
```

```python
import functools

import jax
import jax.numpy as jnp
from jax import lax
from jax.experimental import pallas as pl
from jax.experimental.pallas import tpu as pltpu
from jax.sharding import PartitionSpec as P

MESH = pl.DeviceIdType.MESH
f32, bf16 = jnp.float32, jnp.bfloat16
WIDTH = 128


def split(value):
    high = value.astype(bf16)
    return high, (value - high.astype(f32)).astype(bf16)


def dot3(a, b):
    (a_high, a_low), (b_high, b_low) = a, b
    left = jnp.concatenate([a_high, a_low, a_high], axis=1)
    right = jnp.concatenate([b_high, b_high, b_low], axis=0)
    return jnp.dot(left, right, preferred_element_type=f32)


NEAR = 64
LOW0, UP0, LOW1, UP1, EXTRA = range(5)


def kernel(
    count, ring, bounds_ref, x_ref, vec_ref, fac_ref, out_ref,
    wide, narrow, wide_box, narrow_box, upper_high, upper_low, lower_high, lower_low, extra_high, extra_low,
    cross, crossed, cross_high, cross_low,
    window, below, tops, partner, nearby, local,
    shift_send, shift_recv, hop_send, hop_recv, cross_send, cross_recv,
    first_send, first_recv, up_send, up_recv, over_send, over_recv, near_send, near_recv,
):
    me, slab = lax.axis_index("row"), lax.axis_index("col")
    bw = x_ref.shape[0] // 2
    part = bw // ring
    pairs, width = below.shape[1], WIDTH
    pieces = 2 * pairs
    first, last = me == 0, me == count - 1
    inner = jnp.logical_not(first)
    odd = lax.rem(me, 2) == 1
    even = jnp.logical_not(odd)
    early = me >= count - 4

    def block_rows(owner):
        return pl.ds(pl.multiple_of(owner * part, part), part)

    def columns(p):
        return pl.ds(pl.multiple_of(p * width, width), width)

    def lanes(p):
        return columns(lax.rem(p, 2))

    def broad(q):
        return pl.ds(pl.multiple_of(q * 2 * width, 2 * width), 2 * width)

    barrier = pltpu.get_barrier_semaphore()

    @pl.when(inner)
    def _():
        pl.semaphore_signal(barrier, inc=1, device_id={"row": me - 1}, device_id_type=MESH)

    @pl.when(jnp.logical_not(last))
    def _():
        pl.semaphore_signal(barrier, inc=1, device_id={"row": me + 1}, device_id_type=MESH)

    @pl.when(odd & (me > 1))
    def _():
        pl.semaphore_signal(barrier, inc=1, device_id={"row": me - 2}, device_id_type=MESH)

    @pl.when(odd & (me + 2 < count))
    def _():
        pl.semaphore_signal(barrier, inc=1, device_id={"row": me + 2}, device_id_type=MESH)

    for way in range(2):
        @pl.when(slab + 1 < ring if way == 0 else slab >= 1)
        def _():
            pl.semaphore_signal(
                barrier, inc=1, device_id={"col": slab + (1 - 2 * way)}, device_id_type=MESH
            )

    def triangles(s, b):
        w = vec_ref[s, b]
        return w[:, :bw] + w[:, bw:]

    def diagonal(s, b):
        f = fac_ref[s, b]
        return sum(
            jnp.where(slab * part // NEAR == k, f[:, k * NEAR:(k + 1) * NEAR], 0.0)
            for k in range(bw // NEAR)
        )

    mine = block_rows(slab)
    narrow_box[...] = triangles(0, 0)
    wide_box[0, :, :bw], wide_box[1, :, :bw] = triangles(0, 1), triangles(1, 1)
    wide_box[0, :, bw:] = jnp.concatenate([diagonal(0, 1), diagonal(0, 0)], axis=1)
    wide_box[1, :, bw:] = jnp.concatenate([diagonal(1, 0), diagonal(1, 1)], axis=1)
    narrow[1, mine] = triangles(1, 0)

    @pl.when(last)
    def _():
        wide[2, mine, :bw] = triangles(0, 0)
        wide[2, mine, bw:] = jnp.concatenate([diagonal(0, 0)] * 2, axis=1)

    @pl.when(first)
    def _():
        wide[1, mine, :bw] = jnp.zeros((part, bw), f32)
        wide[1, mine, bw:] = jnp.concatenate([diagonal(1, 0)] * 2, axis=1)
        window[0] = jnp.zeros_like(window[0])

    def greeted(there):
        return jnp.where(there, 1, 0)

    pl.semaphore_wait(
        barrier,
        greeted(me > 0) + greeted(me < count - 1) + greeted(slab > 0) + greeted(slab < ring - 1)
        + greeted(odd & (me > 1)) + greeted(odd & (me + 2 < count)),
    )

    place = {LOW0: wide.at[0], UP0: narrow.at[0], LOW1: narrow.at[1], UP1: wide.at[1], EXTRA: wide.at[2]}
    moved = ((LOW0, wide_box.at[0]), (UP0, narrow_box), (UP1, wide_box.at[1]))

    def shift(k):
        slot, box = moved[k]
        return pltpu.make_async_remote_copy(
            src_ref=box, dst_ref=place[slot].at[mine],
            send_sem=shift_send.at[k], recv_sem=shift_recv.at[k],
            device_id={"row": me + 1}, device_id_type=MESH,
        )

    def initial(h, p):
        return pltpu.make_async_remote_copy(
            src_ref=x_ref.at[pl.ds(h * bw, bw), columns(p)], dst_ref=window.at[h, p // 2, :, lanes(p)],
            send_sem=first_send.at[h, p], recv_sem=first_recv.at[h, p],
            device_id={"row": me + 1}, device_id_type=MESH,
        )

    def hop(way, slot, t, owner):
        block = place[slot].at[block_rows(owner)]
        return pltpu.make_async_remote_copy(
            src_ref=block, dst_ref=block,
            send_sem=hop_send.at[way, slot, t], recv_sem=hop_recv.at[way, slot, t],
            device_id={"col": slab + (1 - 2 * way)}, device_id_type=MESH,
        )

    def sends(way, t):
        if way == 0:
            return (slab - t >= 0) & (slab + 1 < ring)
        return (slab + t < ring) & (slab >= 1)

    def gets(way, t):
        return slab - 1 - t >= 0 if way == 0 else slab + 1 + t < ring

    def send_hops(slot, t, when):
        for way in range(2):
            @pl.when(when & (t < ring - 1) & sends(way, t))
            def _():
                hop(way, slot, t, slab - (1 - 2 * way) * t).start()

    def get_hops(slot, t, when):
        for way in range(2):
            @pl.when(when & gets(way, t))
            def _():
                hop(way, slot, t, slab - (1 - 2 * way) * (t + 1)).wait_recv()

    send_hops(EXTRA, 0, last)

    @pl.when(jnp.logical_not(last))
    def _():
        for k in range(len(moved)):
            shift(k).start()
        for p in range(pieces):
            for h in range(2):
                initial(h, p).start()

    for k, slot in enumerate((LOW0, UP0)):
        @pl.when(inner)
        def _():
            shift(k).wait_recv()

        send_hops(slot, 0, inner)

    for t in range(ring - 1):
        for slot in (EXTRA, LOW0, UP0):
            if t == ring - 2 and slot == UP0:
                break
            when = last if slot == EXTRA else inner
            get_hops(slot, t, when)
            send_hops(slot, t + 1, when)

    always = slab >= 0
    send_hops(LOW1, 0, always)

    @pl.when(inner)
    def _():
        shift(2).wait_recv()
        both = wide[1, mine, bw:]
        lane = lax.broadcasted_iota(jnp.int32, both.shape, 1)
        wide[1, mine, bw:] = jnp.where(lane < NEAR, wide_box[1, :, bw:], both)

    send_hops(UP1, 0, always)

    def second(k):
        t, slot = k // 2, (LOW1, UP1)[k % 2]
        get_hops(slot, t, always)
        send_hops(slot, t + 1, always)

    def whole(slot, s, block):
        row = lax.broadcasted_iota(jnp.int32, (bw, bw), 0)
        col = lax.broadcasted_iota(jnp.int32, (bw, bw), 1)
        row2 = lax.broadcasted_iota(jnp.int32, (2 * bw, 2 * bw), 0)
        col2 = lax.broadcasted_iota(jnp.int32, (2 * bw, 2 * bw), 1)
        unit = jnp.where(row2 == col2, 1.0, 0.0).astype(f32)
        start = block * bw
        live = (start >= bounds_ref[s, 0]) & (start <= bounds_ref[s, 1])
        packed = place[slot][:, :bw]
        near = place[EXTRA if slot == EXTRA else (LOW0, UP1)[s]][:, bw:]
        if slot in (UP0, UP1):
            near = near[:, NEAR:]
        else:
            near = near[:, :NEAR]
        near = near * jnp.where(live, 1.0, 0.0).astype(f32)
        w = jnp.concatenate(
            [jnp.where(col >= row, packed, 0.0), jnp.where(col < row, packed, 0.0)], axis=1
        )
        w_high, w_low = split(w)
        turned = (w_high.T, w_low.T)
        gram = dot3((w_high, w_low), turned)
        factor = jnp.where(
            row // NEAR == col // NEAR, jnp.concatenate([near] * (bw // NEAR), axis=1), 0.0
        )
        size = NEAR
        while size < bw:
            cross_part = (row // (2 * size) == col // (2 * size)) & (row // size < col // size)
            parts = split(factor)
            right = dot3(split(jnp.where(cross_part, gram, 0.0)), parts)
            factor = factor - dot3(parts, split(right))
            size *= 2
        g = dot3(split(factor), (w_high, w_low))
        return unit - dot3(turned, split(g))

    def build_low(s):
        lower_high[s], lower_low[s] = split(whole(2 * s, s, 2 * me - 1 + s))

    def build_up(s):
        q = whole(2 * s + 1, s, 2 * me - 2 + s)
        mixed = dot3(split(q[:, bw:]), (lower_high[s, :bw], lower_low[s, :bw]))
        upper_high[s, :, :bw], upper_low[s, :, :bw] = split(q[:, :bw])
        upper_high[s, :, bw:], upper_low[s, :, bw:] = split(mixed)

        @pl.when(even & inner)
        def _():
            cross[s] = mixed[:bw, bw:]
            across(s).start()

    def across(s):
        return pltpu.make_async_remote_copy(
            src_ref=cross.at[s], dst_ref=crossed.at[s],
            send_sem=cross_send.at[s], recv_sem=cross_recv.at[s],
            device_id={"row": me + 1}, device_id_type=MESH,
        )

    def get_across(s):
        @pl.when(odd & (me > 1))
        def _():
            across(s).wait_recv()
            cross_high[s], cross_low[s] = split(crossed[s])

    @pl.when(last)
    def _():
        extra_high[...], extra_low[...] = split(whole(EXTRA, 0, 2 * me))

        def own(p, carry):
            both = dot3((extra_high[...], extra_low[...]), split(x_ref[:, broad(p)]))
            below[0, p], below[1, p] = both[:bw], both[bw:]
            return carry

        lax.fori_loop(0, pairs, own, 0)

    @pl.when(inner)
    def _():
        build_low(0)

    get_hops(UP0, ring - 2, inner)

    @pl.when(inner)
    def _():
        build_up(0)

    steps = 2 * (ring - 1)

    @pl.when(jnp.logical_not(early))
    def _():
        for k in range(steps):
            second(k)
        build_low(1)
        build_up(1)

    def up(s, p):
        block = (s, p // 2, slice(None), lanes(p))
        return pltpu.make_async_remote_copy(
            src_ref=tops.at[block], dst_ref=below.at[block],
            send_sem=up_send.at[s, p], recv_sem=up_recv.at[s, p],
            device_id={"row": me - 2}, device_id_type=MESH,
        )

    def over(s, p):
        block = (s, p // 2, slice(None), lanes(p))
        return pltpu.make_async_remote_copy(
            src_ref=partner.at[block], dst_ref=below.at[block],
            send_sem=over_send.at[s, p], recv_sem=over_recv.at[s, p],
            device_id={"row": me - 1}, device_id_type=MESH,
        )

    def near(s, q):
        return pltpu.make_async_remote_copy(
            src_ref=partner.at[s, q], dst_ref=nearby.at[s, q],
            send_sem=near_send.at[s, q], recv_sem=near_recv.at[s, q],
            device_id={"row": me + 1}, device_id_type=MESH,
        )

    def get_initial(q):
        for h in range(2):
            for i in range(2):
                initial(h, 2 * q + i).wait_recv()

    def second_at(p):
        for k in range(min(steps, pieces - 2)):
            @pl.when(early & (p == k + 1))
            def _():
                second(k)

    def share(s, q):
        parts = split(jnp.concatenate([window[0, q], window[1, q]], axis=0))
        return dot3((upper_high[s, :bw, :2 * bw], upper_low[s, :bw, :2 * bw]), parts)

    def settle(s, q):
        parts = split(jnp.concatenate([window[0, q], window[1, q], below[s, q]], axis=0))
        kept = dot3((upper_high[s, bw:], upper_low[s, bw:]), parts)
        ended = dot3((lower_high[s, bw:], lower_low[s, bw:]), tuple(value[bw:] for value in parts))
        if s == 0:
            window[0, q], window[1, q] = kept, ended
        else:
            out_ref[:bw, broad(q)], out_ref[bw:, broad(q)] = kept, ended

    def odd_sweep(s):
        def pair(q, carry):
            if s == 0:
                get_initial(q)
            local[...] = share(s, q)

            @pl.when(me > 1)
            def _():
                near(s, q).wait_recv()

            for i in range(2):
                p = 2 * q + i
                half_lanes = slice(i * width, (i + 1) * width)

                @pl.when(jnp.logical_not(last))
                def _():
                    up(s, p).wait_recv()

                step = (upper_high[s, :bw, 2 * bw:], upper_low[s, :bw, 2 * bw:])
                mine = local[:, half_lanes] + dot3(step, split(below[s, q, :, half_lanes]))
                partner[s, q, :, half_lanes] = mine

                @pl.when(me > 1)
                def _():
                    step = (cross_high[s], cross_low[s])
                    tops[s, q, :, half_lanes] = nearby[s, q, :, half_lanes] + dot3(step, split(mine))
                    up(s, p).start()

                over(s, p).start()
                if s == 0:
                    second_at(p)

            settle(s, q)
            return carry

        lax.fori_loop(0, pairs, pair, 0)

    def even_sweep(s):
        def pair(q, carry):
            @pl.when((q < pairs) & inner)
            def _():
                if s == 0:
                    get_initial(q)
                partner[s, q] = share(s, q)
                near(s, q).start()

            if s == 0:
                second_at(2 * q - 1)
                second_at(2 * q)

            @pl.when(q >= 1)
            def _():
                over(s, 2 * q - 2).wait_recv()
                over(s, 2 * q - 1).wait_recv()
                if s == 1:
                    settle(s, q - 1)

            if s == 0:
                @pl.when((q >= 1) & inner)
                def _():
                    settle(s, q - 1)

                @pl.when((q >= 1) & first)
                def _():
                    window[1, q - 1] = below[0, q - 1]

            return carry

        lax.fori_loop(0, pairs + 1, pair, 0)

    def sweep(s):
        get_across(s)

        @pl.when(odd)
        def _():
            odd_sweep(s)

        @pl.when(even)
        def _():
            even_sweep(s)

    sweep(0)

    @pl.when(early)
    def _():
        for k in range(min(steps, pieces - 2), steps):
            second(k)
        build_low(1)
        build_up(1)

    sweep(1)

    for slot, when in ((LOW0, inner), (UP0, inner), (LOW1, always), (UP1, always), (EXTRA, last)):
        for t in range(ring - 1):
            for way in range(2):
                @pl.when(when & sends(way, t))
                def _():
                    hop(way, slot, t, slab).wait_send()

    @pl.when(jnp.logical_not(last))
    def _():
        for k in range(len(moved)):
            shift(k).wait_send()

    @pl.when(even & inner)
    def _():
        across(0).wait_send()
        across(1).wait_send()

    def finish(p, carry):
        for s in range(2):
            @pl.when(odd & (me > 1))
            def _():
                up(s, p).wait_send()

            @pl.when(odd)
            def _():
                over(s, p).wait_send()

            @pl.when(even & inner & (p < pairs))
            def _():
                near(s, p).wait_send()

        @pl.when(jnp.logical_not(last))
        def _():
            initial(0, p).wait_send()
            initial(1, p).wait_send()

        return carry

    lax.fori_loop(0, pieces, finish, 0)


def per_device(singular_vectors, reflector_vectors, reflector_factors, sweep_bounds):
    count, ring = lax.axis_size("row"), lax.axis_size("col")
    rows, cols = singular_vectors.shape
    sweeps, blocks, _, span = reflector_vectors.shape
    bw = span // 2
    assert sweeps == 2 and blocks == 2 and rows == span and cols % (2 * WIDTH) == 0
    assert count % 2 == 0
    pairs = cols // (2 * WIDTH)
    vmem, dma = pltpu.VMEM, pltpu.SemaphoreType.DMA
    return pl.pallas_call(
        functools.partial(kernel, count, ring),
        out_shape=jax.ShapeDtypeStruct((rows, cols), f32),
        in_specs=[pl.BlockSpec(memory_space=pltpu.SMEM)] + [pl.BlockSpec(memory_space=vmem)] * 3,
        out_specs=pl.BlockSpec(memory_space=vmem),
        scratch_shapes=[
            vmem((3, bw, bw + 2 * NEAR), f32), vmem((2, bw, bw), f32),
            vmem((2, bw // ring, bw + 2 * NEAR), f32), vmem((bw // ring, bw), f32),
            vmem((2, span, 3 * bw), bf16), vmem((2, span, 3 * bw), bf16),
            vmem((2, span, span), bf16), vmem((2, span, span), bf16),
            vmem((span, span), bf16), vmem((span, span), bf16),
            vmem((2, bw, bw), f32), vmem((2, bw, bw), f32),
            vmem((2, bw, bw), bf16), vmem((2, bw, bw), bf16),
            vmem((2, pairs, bw, 2 * WIDTH), f32),
            vmem((2, pairs, bw, 2 * WIDTH), f32),
            vmem((2, pairs, bw, 2 * WIDTH), f32),
            vmem((2, pairs, bw, 2 * WIDTH), f32),
            vmem((2, pairs, bw, 2 * WIDTH), f32),
            vmem((bw, 2 * WIDTH), f32),
            dma((3,)), dma((3,)), dma((2, 5, ring)), dma((2, 5, ring)),
            dma((2,)), dma((2,)),
            dma((2, 2 * pairs)), dma((2, 2 * pairs)), dma((2, 2 * pairs)), dma((2, 2 * pairs)),
            dma((2, 2 * pairs)), dma((2, 2 * pairs)), dma((2, pairs)), dma((2, pairs)),
        ],
        compiler_params=pltpu.CompilerParams(
            collective_id=0, has_side_effects=True, vmem_limit_bytes=56 * 2**20
        ),
    )(sweep_bounds, singular_vectors, reflector_vectors, reflector_factors)


def solution(mesh):
    placed = (P("row", "col"), P(None, "row", "col", None), P(None, "row", "col", None), P())
    return jax.shard_map(
        per_device, mesh=mesh, in_specs=placed, out_specs=P("row", "col"), check_vma=False
    )
```

```python
import functools

import jax
import jax.numpy as jnp
from jax import lax
from jax.experimental import pallas as pl
from jax.experimental.pallas import tpu as pltpu
from jax.sharding import PartitionSpec as P

MESH = pl.DeviceIdType.MESH
f32, bf16 = jnp.float32, jnp.bfloat16
WIDTH = 128


def split(value):
    high = value.astype(bf16)
    return high, (value - high.astype(f32)).astype(bf16)


def dot3(a, b):
    (a_high, a_low), (b_high, b_low) = a, b
    left = jnp.concatenate([a_high, a_low, a_high], axis=1)
    right = jnp.concatenate([b_high, b_high, b_low], axis=0)
    return jnp.dot(left, right, preferred_element_type=f32)


NEAR = 64
LOW0, UP0, LOW1, UP1, EXTRA = range(5)


def kernel(
    count, ring, bounds_ref, x_ref, vec_ref, fac_ref, out_ref,
    wide, narrow, wide_box, narrow_box, upper_high, upper_low, lower_high, lower_low, extra_high, extra_low,
    cross, crossed, cross_high, cross_low,
    window, below, tops, partner, nearby, local,
    shift_send, shift_recv, hop_send, hop_recv, cross_send, cross_recv,
    first_send, first_recv, up_send, up_recv, over_send, over_recv, near_send, near_recv,
):
    me, slab = lax.axis_index("row"), lax.axis_index("col")
    bw = x_ref.shape[0] // 2
    half = bw // 2
    part = bw // ring
    pairs, width = below.shape[1], WIDTH
    pieces = 2 * pairs
    first, last = me == 0, me == count - 1
    inner = jnp.logical_not(first)
    odd = lax.rem(me, 2) == 1
    even = jnp.logical_not(odd)
    early = me >= count - 4

    def block_rows(owner):
        return pl.ds(pl.multiple_of(owner * part, part), part)

    def columns(p):
        return pl.ds(pl.multiple_of(p * width, width), width)

    def lanes(p):
        return columns(lax.rem(p, 2))

    def broad(q):
        return pl.ds(pl.multiple_of(q * 2 * width, 2 * width), 2 * width)

    barrier = pltpu.get_barrier_semaphore()

    @pl.when(inner)
    def _():
        pl.semaphore_signal(barrier, inc=1, device_id={"row": me - 1}, device_id_type=MESH)

    @pl.when(jnp.logical_not(last))
    def _():
        pl.semaphore_signal(barrier, inc=1, device_id={"row": me + 1}, device_id_type=MESH)

    @pl.when(odd & (me > 1))
    def _():
        pl.semaphore_signal(barrier, inc=1, device_id={"row": me - 2}, device_id_type=MESH)

    @pl.when(odd & (me + 2 < count))
    def _():
        pl.semaphore_signal(barrier, inc=1, device_id={"row": me + 2}, device_id_type=MESH)

    for way in range(2):
        @pl.when(slab + 1 < ring if way == 0 else slab >= 1)
        def _():
            pl.semaphore_signal(
                barrier, inc=1, device_id={"col": slab + (1 - 2 * way)}, device_id_type=MESH
            )

    def triangles(s, b):
        w = vec_ref[s, b]
        return w[:, :bw] + w[:, bw:]

    def diagonal(s, b):
        f = fac_ref[s, b]
        return sum(
            jnp.where(slab * part // NEAR == k, f[:, k * NEAR:(k + 1) * NEAR], 0.0)
            for k in range(bw // NEAR)
        )

    mine = block_rows(slab)
    narrow_box[...] = triangles(0, 0)
    wide_box[0, :, :bw], wide_box[1, :, :bw] = triangles(0, 1), triangles(1, 1)
    wide_box[0, :, bw:] = jnp.concatenate([diagonal(0, 1), diagonal(0, 0)], axis=1)
    wide_box[1, :, bw:] = jnp.concatenate([diagonal(1, 0), diagonal(1, 1)], axis=1)
    narrow[1, mine] = triangles(1, 0)

    @pl.when(last)
    def _():
        wide[2, mine, :bw] = triangles(0, 0)
        wide[2, mine, bw:] = jnp.concatenate([diagonal(0, 0)] * 2, axis=1)

    @pl.when(first)
    def _():
        wide[1, mine, :bw] = jnp.zeros((part, bw), f32)
        wide[1, mine, bw:] = jnp.concatenate([diagonal(1, 0)] * 2, axis=1)
        window[0] = jnp.zeros_like(window[0])

    def greeted(there):
        return jnp.where(there, 1, 0)

    pl.semaphore_wait(
        barrier,
        greeted(me > 0) + greeted(me < count - 1) + greeted(slab > 0) + greeted(slab < ring - 1)
        + greeted(odd & (me > 1)) + greeted(odd & (me + 2 < count)),
    )

    place = {LOW0: wide.at[0], UP0: narrow.at[0], LOW1: narrow.at[1], UP1: wide.at[1], EXTRA: wide.at[2]}
    moved = ((LOW0, wide_box.at[0]), (UP0, narrow_box), (UP1, wide_box.at[1]))

    def shift(k):
        slot, box = moved[k]
        return pltpu.make_async_remote_copy(
            src_ref=box, dst_ref=place[slot].at[mine],
            send_sem=shift_send.at[k], recv_sem=shift_recv.at[k],
            device_id={"row": me + 1}, device_id_type=MESH,
        )

    def initial(h, p):
        return pltpu.make_async_remote_copy(
            src_ref=x_ref.at[pl.ds(h * bw, bw), columns(p)], dst_ref=window.at[h, p // 2, :, lanes(p)],
            send_sem=first_send.at[h, p], recv_sem=first_recv.at[h, p],
            device_id={"row": me + 1}, device_id_type=MESH,
        )

    def hop(way, slot, t, owner):
        block = place[slot].at[block_rows(owner)]
        return pltpu.make_async_remote_copy(
            src_ref=block, dst_ref=block,
            send_sem=hop_send.at[way, slot, t], recv_sem=hop_recv.at[way, slot, t],
            device_id={"col": slab + (1 - 2 * way)}, device_id_type=MESH,
        )

    def sends(way, t):
        if way == 0:
            return (slab - t >= 0) & (slab + 1 < ring)
        return (slab + t < ring) & (slab >= 1)

    def gets(way, t):
        return slab - 1 - t >= 0 if way == 0 else slab + 1 + t < ring

    def send_hops(slot, t, when):
        for way in range(2):
            @pl.when(when & (t < ring - 1) & sends(way, t))
            def _():
                hop(way, slot, t, slab - (1 - 2 * way) * t).start()

    def get_hops(slot, t, when):
        for way in range(2):
            @pl.when(when & gets(way, t))
            def _():
                hop(way, slot, t, slab - (1 - 2 * way) * (t + 1)).wait_recv()

    send_hops(EXTRA, 0, last)

    @pl.when(jnp.logical_not(last))
    def _():
        for k in range(len(moved)):
            shift(k).start()
        for p in range(pieces):
            for h in range(2):
                initial(h, p).start()

    for k, slot in enumerate((LOW0, UP0)):
        @pl.when(inner)
        def _():
            shift(k).wait_recv()

        send_hops(slot, 0, inner)

    for t in range(ring - 2):
        for slot in (EXTRA, LOW0, UP0):
            when = last if slot == EXTRA else inner
            get_hops(slot, t, when)
            send_hops(slot, t + 1, when)

    always = slab >= 0
    send_hops(LOW1, 0, always)

    @pl.when(inner)
    def _():
        shift(2).wait_recv()
        both = wide[1, mine, bw:]
        lane = lax.broadcasted_iota(jnp.int32, both.shape, 1)
        wide[1, mine, bw:] = jnp.where(lane < NEAR, wide_box[1, :, bw:], both)

    send_hops(UP1, 0, always)

    def second(k):
        t, slot = k // 2, (LOW1, UP1)[k % 2]
        get_hops(slot, t, always)
        send_hops(slot, t + 1, always)

    def stages(slot, s, block):
        row = lax.broadcasted_iota(jnp.int32, (bw, bw), 0)
        col = lax.broadcasted_iota(jnp.int32, (bw, bw), 1)
        row2 = lax.broadcasted_iota(jnp.int32, (2 * bw, 2 * bw), 0)
        col2 = lax.broadcasted_iota(jnp.int32, (2 * bw, 2 * bw), 1)
        unit = jnp.where(row2 == col2, 1.0, 0.0).astype(f32)
        start = block * bw
        live = (start >= bounds_ref[s, 0]) & (start <= bounds_ref[s, 1])
        packed = place[slot][:, :bw]
        near = place[EXTRA if slot == EXTRA else (LOW0, UP1)[s]][:, bw:]
        if slot in (UP0, UP1):
            near = near[:, NEAR:]
        else:
            near = near[:, :NEAR]
        near = near * jnp.where(live, 1.0, 0.0).astype(f32)
        w = jnp.concatenate(
            [jnp.where(col >= row, packed, 0.0), jnp.where(col < row, packed, 0.0)], axis=1
        )
        w_high, w_low = split(w)
        turned = (w_high.T, w_low.T)
        yield
        gram = dot3((w_high[:bw - NEAR], w_low[:bw - NEAR]), turned)
        yield
        wide_near = jnp.concatenate([near] * (bw // NEAR), axis=1)
        factor = jnp.where(row // NEAR == col // NEAR, wide_near, 0.0)
        upper, lower = slice(0, NEAR), slice(half, half + NEAR)
        beside = jnp.concatenate([gram[upper], gram[lower]], axis=0)
        near_row, near_col = row[:half] // NEAR, col[:half] // NEAR
        beside = jnp.where(near_col == 2 * near_row + 1, beside, 0.0)
        right = dot3(split(beside), split(factor))
        yield
        outer = jnp.concatenate([wide_near[upper], wide_near[lower]], axis=0)[:, :half]
        outer = jnp.where(near_row[:, :half] == near_col[:, :half], outer, 0.0)
        change = dot3(split(outer), split(right))
        yield
        nothing = jnp.zeros((NEAR, bw), f32)
        factor = factor - jnp.concatenate(
            [change[:NEAR], nothing, change[NEAR:], nothing], axis=0
        )
        g_tail = dot3(split(factor[half:, half:]), (w_high[half:], w_low[half:]))
        yield
        rest = w[:half] - dot3(split(gram[:half, half:]), split(g_tail))
        yield
        g_head = dot3(split(factor[:half, :half]), split(rest))
        yield
        g = jnp.concatenate([g_head, g_tail], axis=0)
        return unit - dot3(turned, split(g))

    def in_step(*blocks):
        results = [None] * len(blocks)
        waiting = list(enumerate(blocks))
        while waiting:
            for item in tuple(waiting):
                try:
                    next(item[1])
                except StopIteration as end:
                    results[item[0]] = end.value
                    waiting.remove(item)
        return results

    def build(s):
        q_low, q = in_step(
            stages((LOW0, LOW1)[s], s, 2 * me - 1 + s), stages((UP0, UP1)[s], s, 2 * me - 2 + s)
        )
        lower_high[s], lower_low[s] = split(q_low[bw:])
        mixed = dot3(split(q[:, bw:]), split(q_low[:bw]))
        upper_high[s, :, :bw], upper_low[s, :, :bw] = split(q[:, :bw])
        upper_high[s, :, bw:], upper_low[s, :, bw:] = split(mixed)

        @pl.when(even & inner)
        def _():
            cross[s] = mixed[:bw, bw:]
            across(s).start()

    def across(s):
        return pltpu.make_async_remote_copy(
            src_ref=cross.at[s], dst_ref=crossed.at[s],
            send_sem=cross_send.at[s], recv_sem=cross_recv.at[s],
            device_id={"row": me + 1}, device_id_type=MESH,
        )

    def get_across(s):
        @pl.when(odd & (me > 1))
        def _():
            across(s).wait_recv()
            cross_high[s], cross_low[s] = split(crossed[s])

    get_hops(EXTRA, ring - 2, last)

    @pl.when(last)
    def _():
        extra_high[...], extra_low[...] = split(in_step(stages(EXTRA, 0, 2 * me))[0])

        def own(p, carry):
            both = dot3((extra_high[...], extra_low[...]), split(x_ref[:, broad(p)]))
            below[0, p], below[1, p] = both[:bw], both[bw:]
            return carry

        lax.fori_loop(0, pairs, own, 0)

    get_hops(LOW0, ring - 2, inner)

    get_hops(UP0, ring - 2, inner)

    @pl.when(inner)
    def _():
        build(0)

    steps = 2 * (ring - 1)

    @pl.when(jnp.logical_not(early))
    def _():
        for k in range(steps):
            second(k)
        build(1)

    def up(s, p):
        block = (s, p // 2, slice(None), lanes(p))
        return pltpu.make_async_remote_copy(
            src_ref=tops.at[block], dst_ref=below.at[block],
            send_sem=up_send.at[s, p], recv_sem=up_recv.at[s, p],
            device_id={"row": me - 2}, device_id_type=MESH,
        )

    def over(s, p):
        block = (s, p // 2, slice(None), lanes(p))
        return pltpu.make_async_remote_copy(
            src_ref=partner.at[block], dst_ref=below.at[block],
            send_sem=over_send.at[s, p], recv_sem=over_recv.at[s, p],
            device_id={"row": me - 1}, device_id_type=MESH,
        )

    def near(s, q):
        return pltpu.make_async_remote_copy(
            src_ref=partner.at[s, q], dst_ref=nearby.at[s, q],
            send_sem=near_send.at[s, q], recv_sem=near_recv.at[s, q],
            device_id={"row": me + 1}, device_id_type=MESH,
        )

    def get_initial(q):
        for h in range(2):
            for i in range(2):
                initial(h, 2 * q + i).wait_recv()

    def second_at(p):
        for k in range(min(steps, pieces - 2)):
            @pl.when(early & (p == k + 1))
            def _():
                second(k)

    def share(s, q):
        parts = split(jnp.concatenate([window[0, q], window[1, q]], axis=0))
        return dot3((upper_high[s, :bw, :2 * bw], upper_low[s, :bw, :2 * bw]), parts)

    def settle(s, q):
        parts = split(jnp.concatenate([window[0, q], window[1, q], below[s, q]], axis=0))
        kept = dot3((upper_high[s, bw:], upper_low[s, bw:]), parts)
        ended = dot3((lower_high[s], lower_low[s]), tuple(value[bw:] for value in parts))
        if s == 0:
            window[0, q], window[1, q] = kept, ended
        else:
            out_ref[:bw, broad(q)], out_ref[bw:, broad(q)] = kept, ended

    def odd_sweep(s):
        def pair(q, carry):
            if s == 0:
                get_initial(q)
            local[...] = share(s, q)

            @pl.when(me > 1)
            def _():
                near(s, q).wait_recv()

            for i in range(2):
                p = 2 * q + i
                half_lanes = slice(i * width, (i + 1) * width)

                @pl.when(jnp.logical_not(last))
                def _():
                    up(s, p).wait_recv()

                step = (upper_high[s, :bw, 2 * bw:], upper_low[s, :bw, 2 * bw:])
                mine = local[:, half_lanes] + dot3(step, split(below[s, q, :, half_lanes]))
                partner[s, q, :, half_lanes] = mine

                @pl.when(me > 1)
                def _():
                    step = (cross_high[s], cross_low[s])
                    tops[s, q, :, half_lanes] = nearby[s, q, :, half_lanes] + dot3(step, split(mine))
                    up(s, p).start()

                over(s, p).start()
                if s == 0:
                    second_at(p)

            settle(s, q)
            return carry

        lax.fori_loop(0, pairs, pair, 0)

    def even_sweep(s):
        def pair(q, carry):
            @pl.when((q < pairs) & inner)
            def _():
                if s == 0:
                    get_initial(q)
                partner[s, q] = share(s, q)
                near(s, q).start()

            if s == 0:
                second_at(2 * q - 1)
                second_at(2 * q)

            @pl.when(q >= 1)
            def _():
                over(s, 2 * q - 2).wait_recv()
                over(s, 2 * q - 1).wait_recv()
                if s == 1:
                    settle(s, q - 1)

            if s == 0:
                @pl.when((q >= 1) & inner)
                def _():
                    settle(s, q - 1)

                @pl.when((q >= 1) & first)
                def _():
                    window[1, q - 1] = below[0, q - 1]

            return carry

        lax.fori_loop(0, pairs + 1, pair, 0)

    def sweep(s):
        get_across(s)

        @pl.when(odd)
        def _():
            odd_sweep(s)

        @pl.when(even)
        def _():
            even_sweep(s)

    sweep(0)

    @pl.when(early)
    def _():
        for k in range(min(steps, pieces - 2), steps):
            second(k)
        build(1)

    sweep(1)

    for slot, when in ((LOW0, inner), (UP0, inner), (LOW1, always), (UP1, always), (EXTRA, last)):
        for t in range(ring - 1):
            for way in range(2):
                @pl.when(when & sends(way, t))
                def _():
                    hop(way, slot, t, slab).wait_send()

    @pl.when(jnp.logical_not(last))
    def _():
        for k in range(len(moved)):
            shift(k).wait_send()

    @pl.when(even & inner)
    def _():
        across(0).wait_send()
        across(1).wait_send()

    def finish(p, carry):
        for s in range(2):
            @pl.when(odd & (me > 1))
            def _():
                up(s, p).wait_send()

            @pl.when(odd)
            def _():
                over(s, p).wait_send()

            @pl.when(even & inner & (p < pairs))
            def _():
                near(s, p).wait_send()

        @pl.when(jnp.logical_not(last))
        def _():
            initial(0, p).wait_send()
            initial(1, p).wait_send()

        return carry

    lax.fori_loop(0, pieces, finish, 0)


def per_device(singular_vectors, reflector_vectors, reflector_factors, sweep_bounds):
    count, ring = lax.axis_size("row"), lax.axis_size("col")
    rows, cols = singular_vectors.shape
    sweeps, blocks, _, span = reflector_vectors.shape
    bw = span // 2
    assert sweeps == 2 and blocks == 2 and rows == span and cols % (2 * WIDTH) == 0
    assert count % 2 == 0 and bw == 4 * NEAR and ring >= 2
    pairs = cols // (2 * WIDTH)
    vmem, dma = pltpu.VMEM, pltpu.SemaphoreType.DMA
    return pl.pallas_call(
        functools.partial(kernel, count, ring),
        out_shape=jax.ShapeDtypeStruct((rows, cols), f32),
        in_specs=[pl.BlockSpec(memory_space=pltpu.SMEM)] + [pl.BlockSpec(memory_space=vmem)] * 3,
        out_specs=pl.BlockSpec(memory_space=vmem),
        scratch_shapes=[
            vmem((3, bw, bw + 2 * NEAR), f32), vmem((2, bw, bw), f32),
            vmem((2, bw // ring, bw + 2 * NEAR), f32), vmem((bw // ring, bw), f32),
            vmem((2, span, 3 * bw), bf16), vmem((2, span, 3 * bw), bf16),
            vmem((2, bw, span), bf16), vmem((2, bw, span), bf16),
            vmem((span, span), bf16), vmem((span, span), bf16),
            vmem((2, bw, bw), f32), vmem((2, bw, bw), f32),
            vmem((2, bw, bw), bf16), vmem((2, bw, bw), bf16),
            vmem((2, pairs, bw, 2 * WIDTH), f32),
            vmem((2, pairs, bw, 2 * WIDTH), f32),
            vmem((2, pairs, bw, 2 * WIDTH), f32),
            vmem((2, pairs, bw, 2 * WIDTH), f32),
            vmem((2, pairs, bw, 2 * WIDTH), f32),
            vmem((bw, 2 * WIDTH), f32),
            dma((3,)), dma((3,)), dma((2, 5, ring)), dma((2, 5, ring)),
            dma((2,)), dma((2,)),
            dma((2, 2 * pairs)), dma((2, 2 * pairs)), dma((2, 2 * pairs)), dma((2, 2 * pairs)),
            dma((2, 2 * pairs)), dma((2, 2 * pairs)), dma((2, pairs)), dma((2, pairs)),
        ],
        compiler_params=pltpu.CompilerParams(
            collective_id=0, has_side_effects=True, vmem_limit_bytes=56 * 2**20
        ),
    )(sweep_bounds, singular_vectors, reflector_vectors, reflector_factors)


def solution(mesh):
    placed = (P("row", "col"), P(None, "row", "col", None), P(None, "row", "col", None), P())
    return jax.shard_map(
        per_device, mesh=mesh, in_specs=placed, out_specs=P("row", "col"), check_vma=False
    )
```

```python
import functools

import jax
import jax.numpy as jnp
from jax import lax
from jax.experimental import pallas as pl
from jax.experimental.pallas import tpu as pltpu
from jax.sharding import PartitionSpec as P

MESH = pl.DeviceIdType.MESH
f32, bf16 = jnp.float32, jnp.bfloat16
WIDTH = 128


def split(value):
    high = value.astype(bf16)
    return high, (value - high.astype(f32)).astype(bf16)


def dot3(a, b):
    (a_high, a_low), (b_high, b_low) = a, b
    left = jnp.concatenate([a_high, a_low, a_high], axis=1)
    right = jnp.concatenate([b_high, b_high, b_low], axis=0)
    return jnp.dot(left, right, preferred_element_type=f32)


NEAR = 64
LOW0, UP0, LOW1, UP1, EXTRA = range(5)


def kernel(
    count, ring, bounds_ref, x_hbm, vec_hbm, fac_hbm, out_ref,
    x_ref, vec_ref, fac_ref, load,
    wide, narrow, wide_box, narrow_box, upper_high, upper_low, lower_high, lower_low, extra_high, extra_low,
    cross, crossed, cross_high, cross_low,
    window, below, tops, partner, nearby, local,
    shift_send, shift_recv, hop_send, hop_recv, cross_send, cross_recv,
    first_send, first_recv, up_send, up_recv, over_send, over_recv, near_send, near_recv,
):
    me, slab = lax.axis_index("row"), lax.axis_index("col")
    bw = x_ref.shape[0] // 2
    half = bw // 2
    part = bw // ring
    pairs, width = below.shape[1], WIDTH
    pieces = 2 * pairs
    first, last = me == 0, me == count - 1
    inner = jnp.logical_not(first)
    odd = lax.rem(me, 2) == 1
    even = jnp.logical_not(odd)
    early = me >= count - 2
    ahead = me < count - 4

    def block_rows(owner):
        return pl.ds(pl.multiple_of(owner * part, part), part)

    def columns(p):
        return pl.ds(pl.multiple_of(p * width, width), width)

    def lanes(p):
        return columns(lax.rem(p, 2))

    def broad(q):
        return pl.ds(pl.multiple_of(q * 2 * width, 2 * width), 2 * width)

    loads = [
        pltpu.make_async_copy(source, target, load.at[k])
        for k, (source, target) in enumerate(
            ((vec_hbm, vec_ref), (fac_hbm, fac_ref), (x_hbm, x_ref))
        )
    ]
    for copy in loads:
        copy.start()

    barrier = pltpu.get_barrier_semaphore()

    @pl.when(inner)
    def _():
        pl.semaphore_signal(barrier, inc=1, device_id={"row": me - 1}, device_id_type=MESH)

    @pl.when(jnp.logical_not(last))
    def _():
        pl.semaphore_signal(barrier, inc=1, device_id={"row": me + 1}, device_id_type=MESH)

    @pl.when(odd & (me > 1))
    def _():
        pl.semaphore_signal(barrier, inc=1, device_id={"row": me - 2}, device_id_type=MESH)

    @pl.when(odd & (me + 2 < count))
    def _():
        pl.semaphore_signal(barrier, inc=1, device_id={"row": me + 2}, device_id_type=MESH)

    for way in range(2):
        @pl.when(slab + 1 < ring if way == 0 else slab >= 1)
        def _():
            pl.semaphore_signal(
                barrier, inc=1, device_id={"col": slab + (1 - 2 * way)}, device_id_type=MESH
            )

    def triangles(s, b):
        w = vec_ref[s, b]
        return w[:, :bw] + w[:, bw:]

    def diagonal(s, b):
        f = fac_ref[s, b]
        return sum(
            jnp.where(slab * part // NEAR == k, f[:, k * NEAR:(k + 1) * NEAR], 0.0)
            for k in range(bw // NEAR)
        )

    loads[0].wait()
    loads[1].wait()
    mine = block_rows(slab)
    narrow_box[...] = triangles(0, 0)
    wide_box[0, :, :bw], wide_box[1, :, :bw] = triangles(0, 1), triangles(1, 1)
    wide_box[0, :, bw:] = jnp.concatenate([diagonal(0, 1), diagonal(0, 0)], axis=1)
    wide_box[1, :, bw:] = jnp.concatenate([diagonal(1, 0), diagonal(1, 1)], axis=1)
    narrow[1, mine] = triangles(1, 0)

    @pl.when(last)
    def _():
        wide[2, mine, :bw] = triangles(0, 0)
        wide[2, mine, bw:] = jnp.concatenate([diagonal(0, 0)] * 2, axis=1)

    @pl.when(first)
    def _():
        wide[1, mine, :bw] = jnp.zeros((part, bw), f32)
        wide[1, mine, bw:] = jnp.concatenate([diagonal(1, 0)] * 2, axis=1)
        window[0] = jnp.zeros_like(window[0])

    def greeted(there):
        return jnp.where(there, 1, 0)

    pl.semaphore_wait(
        barrier,
        greeted(me > 0) + greeted(me < count - 1) + greeted(slab > 0) + greeted(slab < ring - 1)
        + greeted(odd & (me > 1)) + greeted(odd & (me + 2 < count)),
    )

    place = {LOW0: wide.at[0], UP0: narrow.at[0], LOW1: narrow.at[1], UP1: wide.at[1], EXTRA: wide.at[2]}
    moved = ((LOW0, wide_box.at[0]), (UP0, narrow_box), (UP1, wide_box.at[1]))

    def shift(k):
        slot, box = moved[k]
        return pltpu.make_async_remote_copy(
            src_ref=box, dst_ref=place[slot].at[mine],
            send_sem=shift_send.at[k], recv_sem=shift_recv.at[k],
            device_id={"row": me + 1}, device_id_type=MESH,
        )

    def initial(h, p):
        return pltpu.make_async_remote_copy(
            src_ref=x_ref.at[pl.ds(h * bw, bw), columns(p)], dst_ref=window.at[h, p // 2, :, lanes(p)],
            send_sem=first_send.at[h, p], recv_sem=first_recv.at[h, p],
            device_id={"row": me + 1}, device_id_type=MESH,
        )

    def hop(way, slot, t, owner):
        block = place[slot].at[block_rows(owner)]
        return pltpu.make_async_remote_copy(
            src_ref=block, dst_ref=block,
            send_sem=hop_send.at[way, slot, t], recv_sem=hop_recv.at[way, slot, t],
            device_id={"col": slab + (1 - 2 * way)}, device_id_type=MESH,
        )

    def sends(way, t):
        if way == 0:
            return (slab - t >= 0) & (slab + 1 < ring)
        return (slab + t < ring) & (slab >= 1)

    def gets(way, t):
        return slab - 1 - t >= 0 if way == 0 else slab + 1 + t < ring

    def send_hops(slot, t, when):
        for way in range(2):
            @pl.when(when & (t < ring - 1) & sends(way, t))
            def _():
                hop(way, slot, t, slab - (1 - 2 * way) * t).start()

    def get_hops(slot, t, when):
        for way in range(2):
            @pl.when(when & gets(way, t))
            def _():
                hop(way, slot, t, slab - (1 - 2 * way) * (t + 1)).wait_recv()

    send_hops(EXTRA, 0, last)
    loads[2].wait()

    @pl.when(jnp.logical_not(last))
    def _():
        for k in range(len(moved)):
            shift(k).start()
        for p in range(pieces):
            for h in range(2):
                initial(h, p).start()

    for k, slot in enumerate((LOW0, UP0)):
        @pl.when(inner)
        def _():
            shift(k).wait_recv()

        send_hops(slot, 0, inner)

    for t in range(ring - 2):
        for slot in (EXTRA, LOW0, UP0):
            when = last if slot == EXTRA else inner
            get_hops(slot, t, when)
            send_hops(slot, t + 1, when)

    always = slab >= 0
    send_hops(LOW1, 0, always)

    @pl.when(inner)
    def _():
        shift(2).wait_recv()
        both = wide[1, mine, bw:]
        lane = lax.broadcasted_iota(jnp.int32, both.shape, 1)
        wide[1, mine, bw:] = jnp.where(lane < NEAR, wide_box[1, :, bw:], both)

    send_hops(UP1, 0, always)

    def second(k):
        t, slot = k // 2, (LOW1, UP1)[k % 2]
        get_hops(slot, t, always)
        send_hops(slot, t + 1, always)

    def stages(slot, s, block):
        row = lax.broadcasted_iota(jnp.int32, (bw, bw), 0)
        col = lax.broadcasted_iota(jnp.int32, (bw, bw), 1)
        row2 = lax.broadcasted_iota(jnp.int32, (2 * bw, 2 * bw), 0)
        col2 = lax.broadcasted_iota(jnp.int32, (2 * bw, 2 * bw), 1)
        unit = jnp.where(row2 == col2, 1.0, 0.0).astype(f32)
        start = block * bw
        live = (start >= bounds_ref[s, 0]) & (start <= bounds_ref[s, 1])
        packed = place[slot][:, :bw]
        near = place[EXTRA if slot == EXTRA else (LOW0, UP1)[s]][:, bw:]
        if slot in (UP0, UP1):
            near = near[:, NEAR:]
        else:
            near = near[:, :NEAR]
        near = near * jnp.where(live, 1.0, 0.0).astype(f32)
        w = jnp.concatenate(
            [jnp.where(col >= row, packed, 0.0), jnp.where(col < row, packed, 0.0)], axis=1
        )
        w_high, w_low = split(w)
        turned = (w_high.T, w_low.T)
        yield
        gram = dot3((w_high[:bw - NEAR], w_low[:bw - NEAR]), turned)
        yield
        wide_near = jnp.concatenate([near] * (bw // NEAR), axis=1)
        factor = jnp.where(row // NEAR == col // NEAR, wide_near, 0.0)
        upper, lower = slice(0, NEAR), slice(half, half + NEAR)
        beside = jnp.concatenate([gram[upper], gram[lower]], axis=0)
        near_row, near_col = row[:half] // NEAR, col[:half] // NEAR
        beside = jnp.where(near_col == 2 * near_row + 1, beside, 0.0)
        right = dot3(split(beside), split(factor))
        yield
        outer = jnp.concatenate([wide_near[upper], wide_near[lower]], axis=0)[:, :half]
        outer = jnp.where(near_row[:, :half] == near_col[:, :half], outer, 0.0)
        change = dot3(split(outer), split(right))
        yield
        nothing = jnp.zeros((NEAR, bw), f32)
        factor = factor - jnp.concatenate(
            [change[:NEAR], nothing, change[NEAR:], nothing], axis=0
        )
        g_tail = dot3(split(factor[half:, half:]), (w_high[half:], w_low[half:]))
        yield
        rest = w[:half] - dot3(split(gram[:half, half:]), split(g_tail))
        yield
        g_head = dot3(split(factor[:half, :half]), split(rest))
        yield
        g = jnp.concatenate([g_head, g_tail], axis=0)
        return unit - dot3(turned, split(g))

    def in_step(*blocks):
        results = [None] * len(blocks)
        waiting = list(enumerate(blocks))
        while waiting:
            for item in tuple(waiting):
                try:
                    next(item[1])
                except StopIteration as end:
                    results[item[0]] = end.value
                    waiting.remove(item)
        return results

    def build(s):
        q_low, q = in_step(
            stages((LOW0, LOW1)[s], s, 2 * me - 1 + s), stages((UP0, UP1)[s], s, 2 * me - 2 + s)
        )
        lower_high[s], lower_low[s] = split(q_low[bw:])
        mixed = dot3(split(q[:, bw:]), split(q_low[:bw]))
        upper_high[s, :, :bw], upper_low[s, :, :bw] = split(q[:, :bw])
        upper_high[s, :, bw:], upper_low[s, :, bw:] = split(mixed)

        @pl.when(even & inner)
        def _():
            cross[s] = mixed[:bw, bw:]
            across(s).start()

    def across(s):
        return pltpu.make_async_remote_copy(
            src_ref=cross.at[s], dst_ref=crossed.at[s],
            send_sem=cross_send.at[s], recv_sem=cross_recv.at[s],
            device_id={"row": me + 1}, device_id_type=MESH,
        )

    get_hops(EXTRA, ring - 2, last)

    @pl.when(last)
    def _():
        extra_high[...], extra_low[...] = split(in_step(stages(EXTRA, 0, 2 * me))[0])

    def own(q):
        both = dot3((extra_high[...], extra_low[...]), split(x_ref[:, broad(q)]))
        below[0, q], below[1, q] = both[:bw], both[bw:]

    get_hops(LOW0, ring - 2, inner)

    get_hops(UP0, ring - 2, inner)
    steps = 2 * (ring - 1)

    @pl.when(jnp.logical_not(early))
    def _():
        for k in range(steps - 2):
            second(k)

    @pl.when(inner)
    def _():
        build(0)

    @pl.when(ahead)
    def _():
        for k in range(steps - 2, steps):
            second(k)

    @pl.when(ahead)
    def _():
        build(1)

    def up(s, p):
        block = (s, p // 2, slice(None), lanes(p))
        return pltpu.make_async_remote_copy(
            src_ref=tops.at[block], dst_ref=below.at[block],
            send_sem=up_send.at[s, p], recv_sem=up_recv.at[s, p],
            device_id={"row": me - 2}, device_id_type=MESH,
        )

    def over(s, p):
        block = (s, p // 2, slice(None), lanes(p))
        return pltpu.make_async_remote_copy(
            src_ref=partner.at[block], dst_ref=below.at[block],
            send_sem=over_send.at[s, p], recv_sem=over_recv.at[s, p],
            device_id={"row": me - 1}, device_id_type=MESH,
        )

    def near(s, q):
        return pltpu.make_async_remote_copy(
            src_ref=partner.at[s, q], dst_ref=nearby.at[s, q],
            send_sem=near_send.at[s, q], recv_sem=near_recv.at[s, q],
            device_id={"row": me + 1}, device_id_type=MESH,
        )

    def get_initial(q):
        for h in range(2):
            for i in range(2):
                initial(h, 2 * q + i).wait_recv()

    odd_places = ((0, 0), (0, 1), (1, 0), (1, 1), (2, 1))
    even_places = ((1, 1), (2, 1), (3, 0), (3, 0), (3, 0))
    placed = min(steps - 1, len(odd_places)) if pairs >= 4 else 0

    def build_at(q, when):
        @pl.when((q == pairs - 1) & early & when)
        def _():
            for k in range(placed + 1, steps):
                second(k)

        @pl.when((q == pairs - 1) & when)
        def _():
            build(1)

    def second_at(places, q, place):
        for k in range(2):
            @pl.when(jnp.logical_not(early | ahead) & (q == places[k][0]))
            def _():
                if places[k][1] == place:
                    second(steps - 2 + k)

        for k in range(placed):
            if places[k][1] == place:
                @pl.when(early & (q == places[k][0]))
                def _():
                    second(k + 1)

    def share(s, q):
        parts = split(jnp.concatenate([window[0, q], window[1, q]], axis=0))
        return dot3((upper_high[s, :bw, :2 * bw], upper_low[s, :bw, :2 * bw]), parts)

    def settle(s, q):
        parts = split(jnp.concatenate([window[0, q], window[1, q], below[s, q]], axis=0))
        kept = dot3((upper_high[s, bw:], upper_low[s, bw:]), parts)
        ended = dot3((lower_high[s], lower_low[s]), tuple(value[bw:] for value in parts))
        if s == 0:
            window[0, q], window[1, q] = kept, ended
        else:
            out_ref[:bw, broad(q)], out_ref[bw:, broad(q)] = kept, ended

    def carries(s, q, half_lanes):
        step = (upper_high[s, :bw, 2 * bw:], upper_low[s, :bw, 2 * bw:])
        partner[s, q, :, half_lanes] = local[:, half_lanes] + dot3(
            step, split(below[s, q, :, half_lanes])
        )

    def leaving(s, q, half_lanes):
        onward = dot3((cross_high[s], cross_low[s]), split(partner[s, q, :, half_lanes]))
        tops[s, q, :, half_lanes] = nearby[s, q, :, half_lanes] + onward

    def odd_sweep(s):
        def pair(q, carry):
            if s == 0:
                get_initial(q)
            local[...] = share(s, q)

            @pl.when((q == 0) & (me > 1))
            def _():
                across(s).wait_recv()
                cross_high[s], cross_low[s] = split(crossed[s])

            @pl.when(last)
            def _():
                if s == 0:
                    own(q)
                carries(s, q, slice(None))
                near(s, q).wait_recv()
                leaving(s, q, slice(None))
                for i in range(2):
                    up(s, 2 * q + i).start()
                    over(s, 2 * q + i).start()

            @pl.when((me > 1) & jnp.logical_not(last))
            def _():
                near(s, q).wait_recv()

            @pl.when(jnp.logical_not(last))
            def _():
                for i in range(2):
                    p = 2 * q + i
                    half_lanes = slice(i * width, (i + 1) * width)
                    up(s, p).wait_recv()
                    carries(s, q, half_lanes)

                    @pl.when(me > 1)
                    def _():
                        leaving(s, q, half_lanes)
                        up(s, p).start()

                    over(s, p).start()

            if s == 0:
                second_at(odd_places, q, 0)
                build_at(q, jnp.logical_not(ahead))
            settle(s, q)
            if s == 0:
                second_at(odd_places, q, 1)
            return carry

        lax.fori_loop(0, pairs, pair, 0)

    def even_sweep(s):
        def pair(q, carry):
            if s == 0:
                second_at(even_places, q, 0)

            @pl.when((q < pairs) & inner)
            def _():
                if s == 0:
                    get_initial(q)
                partner[s, q] = share(s, q)
                near(s, q).start()

            if s == 0:
                second_at(even_places, q, 1)
                build_at(q, jnp.logical_not(ahead))

            @pl.when(q >= 1)
            def _():
                over(s, 2 * q - 2).wait_recv()
                over(s, 2 * q - 1).wait_recv()
                if s == 1:
                    settle(s, q - 1)

            if s == 0:
                @pl.when((q >= 1) & inner)
                def _():
                    settle(s, q - 1)

                @pl.when((q >= 1) & first)
                def _():
                    window[1, q - 1] = below[0, q - 1]

            return carry

        lax.fori_loop(0, pairs + 1, pair, 0)

    def sweep(s):
        @pl.when(odd)
        def _():
            odd_sweep(s)

        @pl.when(even)
        def _():
            even_sweep(s)

    @pl.when(early)
    def _():
        second(0)

    sweep(0)
    sweep(1)

    for slot, when in ((LOW0, inner), (UP0, inner), (LOW1, always), (UP1, always), (EXTRA, last)):
        for t in range(ring - 1):
            for way in range(2):
                @pl.when(when & sends(way, t))
                def _():
                    hop(way, slot, t, slab).wait_send()

    @pl.when(jnp.logical_not(last))
    def _():
        for k in range(len(moved)):
            shift(k).wait_send()

    @pl.when(even & inner)
    def _():
        across(0).wait_send()
        across(1).wait_send()

    def finish(p, carry):
        for s in range(2):
            @pl.when(odd & (me > 1))
            def _():
                up(s, p).wait_send()

            @pl.when(odd)
            def _():
                over(s, p).wait_send()

            @pl.when(even & inner & (p < pairs))
            def _():
                near(s, p).wait_send()

        @pl.when(jnp.logical_not(last))
        def _():
            initial(0, p).wait_send()
            initial(1, p).wait_send()

        return carry

    lax.fori_loop(0, pieces, finish, 0)


def per_device(singular_vectors, reflector_vectors, reflector_factors, sweep_bounds):
    count, ring = lax.axis_size("row"), lax.axis_size("col")
    rows, cols = singular_vectors.shape
    sweeps, blocks, _, span = reflector_vectors.shape
    bw = span // 2
    assert sweeps == 2 and blocks == 2 and rows == span and cols % (2 * WIDTH) == 0
    pairs = cols // (2 * WIDTH)
    assert count % 2 == 0 and count >= 4 and bw == 4 * NEAR and ring >= 2 and pairs >= 2
    vmem, dma = pltpu.VMEM, pltpu.SemaphoreType.DMA
    return pl.pallas_call(
        functools.partial(kernel, count, ring),
        out_shape=jax.ShapeDtypeStruct((rows, cols), f32),
        in_specs=[pl.BlockSpec(memory_space=pltpu.SMEM)] + [pl.BlockSpec(memory_space=pltpu.HBM)] * 3,
        out_specs=pl.BlockSpec(memory_space=vmem),
        scratch_shapes=[
            vmem((rows, cols), f32), vmem(reflector_vectors.shape, f32),
            vmem(reflector_factors.shape, f32), dma((3,)),
            vmem((3, bw, bw + 2 * NEAR), f32), vmem((2, bw, bw), f32),
            vmem((2, bw // ring, bw + 2 * NEAR), f32), vmem((bw // ring, bw), f32),
            vmem((2, span, 3 * bw), bf16), vmem((2, span, 3 * bw), bf16),
            vmem((2, bw, span), bf16), vmem((2, bw, span), bf16),
            vmem((span, span), bf16), vmem((span, span), bf16),
            vmem((2, bw, bw), f32), vmem((2, bw, bw), f32),
            vmem((2, bw, bw), bf16), vmem((2, bw, bw), bf16),
            vmem((2, pairs, bw, 2 * WIDTH), f32),
            vmem((2, pairs, bw, 2 * WIDTH), f32),
            vmem((2, pairs, bw, 2 * WIDTH), f32),
            vmem((2, pairs, bw, 2 * WIDTH), f32),
            vmem((2, pairs, bw, 2 * WIDTH), f32),
            vmem((bw, 2 * WIDTH), f32),
            dma((3,)), dma((3,)), dma((2, 5, ring)), dma((2, 5, ring)),
            dma((2,)), dma((2,)),
            dma((2, 2 * pairs)), dma((2, 2 * pairs)), dma((2, 2 * pairs)), dma((2, 2 * pairs)),
            dma((2, 2 * pairs)), dma((2, 2 * pairs)), dma((2, pairs)), dma((2, pairs)),
        ],
        compiler_params=pltpu.CompilerParams(
            collective_id=0, has_side_effects=True, vmem_limit_bytes=56 * 2**20
        ),
    )(sweep_bounds, singular_vectors, reflector_vectors, reflector_factors)


def solution(mesh):
    placed = (P("row", "col"), P(None, "row", "col", None), P(None, "row", "col", None), P())
    return jax.shard_map(
        per_device, mesh=mesh, in_specs=placed, out_specs=P("row", "col"), check_vma=False
    )
```

```python
import functools

import jax
import jax.numpy as jnp
from jax import lax
from jax.experimental import pallas as pl
from jax.experimental.pallas import tpu as pltpu
from jax.sharding import PartitionSpec as P

MESH = pl.DeviceIdType.MESH
f32, bf16 = jnp.float32, jnp.bfloat16
WIDTH = 128


def split(value):
    high = value.astype(bf16)
    return high, (value - high.astype(f32)).astype(bf16)


def dot3(a, b):
    (a_high, a_low), (b_high, b_low) = a, b
    left = jnp.concatenate([a_high, a_low, a_high], axis=1)
    right = jnp.concatenate([b_high, b_high, b_low], axis=0)
    return jnp.dot(left, right, preferred_element_type=f32)


NEAR = 64
LOW0, UP0, LOW1, UP1, EXTRA = range(5)


def kernel(
    count, ring, bounds_ref, x_hbm, vec_hbm, fac_hbm, out_ref,
    x_ref, vec_ref, fac_ref, load,
    wide, narrow, wide_box, narrow_box, upper_high, upper_low, lower_high, lower_low, extra_high, extra_low,
    cross, crossed, cross_high, cross_low,
    window, below, tops, partner, nearby, local,
    shift_send, shift_recv, hop_send, hop_recv, cross_send, cross_recv,
    first_send, first_recv, up_send, up_recv, over_send, over_recv, near_send, near_recv,
):
    me, slab = lax.axis_index("row"), lax.axis_index("col")
    bw = x_ref.shape[0] // 2
    half = bw // 2
    part = bw // ring
    pairs, width = below.shape[1], WIDTH
    pieces = 2 * pairs
    first, last = me == 0, me == count - 1
    inner = jnp.logical_not(first)
    odd = lax.rem(me, 2) == 1
    even = jnp.logical_not(odd)
    early = me >= count - 2
    ahead = me < count - 4

    def block_rows(owner):
        return pl.ds(pl.multiple_of(owner * part, part), part)

    def columns(p):
        return pl.ds(pl.multiple_of(p * width, width), width)

    def lanes(p):
        return columns(lax.rem(p, 2))

    def broad(q):
        return pl.ds(pl.multiple_of(q * 2 * width, 2 * width), 2 * width)

    loads = [
        pltpu.make_async_copy(source, target, load.at[k])
        for k, (source, target) in enumerate(
            ((vec_hbm, vec_ref), (fac_hbm, fac_ref), (x_hbm, x_ref))
        )
    ]
    for copy in loads:
        copy.start()

    barrier = pltpu.get_barrier_semaphore()

    @pl.when(inner)
    def _():
        pl.semaphore_signal(barrier, inc=1, device_id={"row": me - 1}, device_id_type=MESH)

    @pl.when(jnp.logical_not(last))
    def _():
        pl.semaphore_signal(barrier, inc=1, device_id={"row": me + 1}, device_id_type=MESH)

    @pl.when(odd & (me > 1))
    def _():
        pl.semaphore_signal(barrier, inc=1, device_id={"row": me - 2}, device_id_type=MESH)

    @pl.when(odd & (me + 2 < count))
    def _():
        pl.semaphore_signal(barrier, inc=1, device_id={"row": me + 2}, device_id_type=MESH)

    for way in range(2):
        @pl.when(slab + 1 < ring if way == 0 else slab >= 1)
        def _():
            pl.semaphore_signal(
                barrier, inc=1, device_id={"col": slab + (1 - 2 * way)}, device_id_type=MESH
            )

    def triangles(s, b):
        w = vec_ref[s, b]
        return w[:, :bw] + w[:, bw:]

    def diagonal(s, b):
        f = fac_ref[s, b]
        return sum(
            jnp.where(slab * part // NEAR == k, f[:, k * NEAR:(k + 1) * NEAR], 0.0)
            for k in range(bw // NEAR)
        )

    loads[0].wait()
    loads[1].wait()
    mine = block_rows(slab)
    narrow_box[...] = triangles(0, 0)
    wide_box[0, :, :bw], wide_box[1, :, :bw] = triangles(0, 1), triangles(1, 1)
    wide_box[0, :, bw:] = jnp.concatenate([diagonal(0, 1), diagonal(0, 0)], axis=1)
    wide_box[1, :, bw:] = jnp.concatenate([diagonal(1, 0), diagonal(1, 1)], axis=1)
    narrow[1, mine] = triangles(1, 0)

    @pl.when(last)
    def _():
        wide[2, mine, :bw] = triangles(0, 0)
        wide[2, mine, bw:] = jnp.concatenate([diagonal(0, 0)] * 2, axis=1)

    @pl.when(first)
    def _():
        wide[1, mine, :bw] = jnp.zeros((part, bw), f32)
        wide[1, mine, bw:] = jnp.concatenate([diagonal(1, 0)] * 2, axis=1)
        window[0] = jnp.zeros_like(window[0])

    def greeted(there):
        return jnp.where(there, 1, 0)

    pl.semaphore_wait(
        barrier,
        greeted(me > 0) + greeted(me < count - 1) + greeted(slab > 0) + greeted(slab < ring - 1)
        + greeted(odd & (me > 1)) + greeted(odd & (me + 2 < count)),
    )

    place = {LOW0: wide.at[0], UP0: narrow.at[0], LOW1: narrow.at[1], UP1: wide.at[1], EXTRA: wide.at[2]}
    moved = ((LOW0, wide_box.at[0]), (UP0, narrow_box), (UP1, wide_box.at[1]))

    def shift(k):
        slot, box = moved[k]
        return pltpu.make_async_remote_copy(
            src_ref=box, dst_ref=place[slot].at[mine],
            send_sem=shift_send.at[k], recv_sem=shift_recv.at[k],
            device_id={"row": me + 1}, device_id_type=MESH,
        )

    def initial(h, p):
        return pltpu.make_async_remote_copy(
            src_ref=x_ref.at[pl.ds(h * bw, bw), columns(p)], dst_ref=window.at[h, p // 2, :, lanes(p)],
            send_sem=first_send.at[h, p], recv_sem=first_recv.at[h, p],
            device_id={"row": me + 1}, device_id_type=MESH,
        )

    def hop(way, slot, t, owner):
        block = place[slot].at[block_rows(owner)]
        return pltpu.make_async_remote_copy(
            src_ref=block, dst_ref=block,
            send_sem=hop_send.at[way, slot, t], recv_sem=hop_recv.at[way, slot, t],
            device_id={"col": slab + (1 - 2 * way)}, device_id_type=MESH,
        )

    def sends(way, t):
        if way == 0:
            return (slab - t >= 0) & (slab + 1 < ring)
        return (slab + t < ring) & (slab >= 1)

    def gets(way, t):
        return slab - 1 - t >= 0 if way == 0 else slab + 1 + t < ring

    def send_hops(slot, t, when):
        for way in range(2):
            @pl.when(when & (t < ring - 1) & sends(way, t))
            def _():
                hop(way, slot, t, slab - (1 - 2 * way) * t).start()

    def get_hops(slot, t, when):
        for way in range(2):
            @pl.when(when & gets(way, t))
            def _():
                hop(way, slot, t, slab - (1 - 2 * way) * (t + 1)).wait_recv()

    send_hops(EXTRA, 0, last)
    loads[2].wait()

    @pl.when(jnp.logical_not(last))
    def _():
        for k in range(len(moved)):
            shift(k).start()
        for p in range(pieces):
            for h in range(2):
                initial(h, p).start()

    for k, slot in enumerate((LOW0, UP0)):
        @pl.when(inner)
        def _():
            shift(k).wait_recv()

        send_hops(slot, 0, inner)

    for t in range(ring - 2):
        for slot in (EXTRA, LOW0, UP0):
            when = last if slot == EXTRA else inner
            get_hops(slot, t, when)
            send_hops(slot, t + 1, when)

    always = slab >= 0
    send_hops(LOW1, 0, always)

    @pl.when(inner)
    def _():
        shift(2).wait_recv()
        both = wide[1, mine, bw:]
        lane = lax.broadcasted_iota(jnp.int32, both.shape, 1)
        wide[1, mine, bw:] = jnp.where(lane < NEAR, wide_box[1, :, bw:], both)

    send_hops(UP1, 0, always)

    def second(k):
        t, slot = k // 2, (LOW1, UP1)[k % 2]
        get_hops(slot, t, always)
        send_hops(slot, t + 1, always)

    def stages(slot, s, block):
        row = lax.broadcasted_iota(jnp.int32, (bw, bw), 0)
        col = lax.broadcasted_iota(jnp.int32, (bw, bw), 1)
        row2 = lax.broadcasted_iota(jnp.int32, (2 * bw, 2 * bw), 0)
        col2 = lax.broadcasted_iota(jnp.int32, (2 * bw, 2 * bw), 1)
        unit = jnp.where(row2 == col2, 1.0, 0.0).astype(f32)
        start = block * bw
        live = (start >= bounds_ref[s, 0]) & (start <= bounds_ref[s, 1])
        packed = place[slot][:, :bw]
        near = place[EXTRA if slot == EXTRA else (LOW0, UP1)[s]][:, bw:]
        if slot in (UP0, UP1):
            near = near[:, NEAR:]
        else:
            near = near[:, :NEAR]
        near = near * jnp.where(live, 1.0, 0.0).astype(f32)
        w = jnp.concatenate(
            [jnp.where(col >= row, packed, 0.0), jnp.where(col < row, packed, 0.0)], axis=1
        )
        w_high, w_low = split(w)
        turned = (w_high.T, w_low.T)
        yield
        gram = dot3((w_high[:bw - NEAR], w_low[:bw - NEAR]), turned)
        yield
        wide_near = jnp.concatenate([near] * (bw // NEAR), axis=1)
        factor = jnp.where(row // NEAR == col // NEAR, wide_near, 0.0)
        upper, lower = slice(0, NEAR), slice(half, half + NEAR)
        beside = jnp.concatenate([gram[upper], gram[lower]], axis=0)
        near_row, near_col = row[:half] // NEAR, col[:half] // NEAR
        beside = jnp.where(near_col == 2 * near_row + 1, beside, 0.0)
        right = dot3(split(beside), split(factor))
        yield
        outer = jnp.concatenate([wide_near[upper], wide_near[lower]], axis=0)[:, :half]
        outer = jnp.where(near_row[:, :half] == near_col[:, :half], outer, 0.0)
        change = dot3(split(outer), split(right))
        yield
        nothing = jnp.zeros((NEAR, bw), f32)
        factor = factor - jnp.concatenate(
            [change[:NEAR], nothing, change[NEAR:], nothing], axis=0
        )
        g_tail = dot3(split(factor[half:, half:]), (w_high[half:], w_low[half:]))
        yield
        rest = w[:half] - dot3(split(gram[:half, half:]), split(g_tail))
        yield
        g_head = dot3(split(factor[:half, :half]), split(rest))
        yield
        g = jnp.concatenate([g_head, g_tail], axis=0)
        return unit - dot3(turned, split(g))

    def in_step(*blocks):
        results = [None] * len(blocks)
        waiting = list(enumerate(blocks))
        while waiting:
            for item in tuple(waiting):
                try:
                    next(item[1])
                except StopIteration as end:
                    results[item[0]] = end.value
                    waiting.remove(item)
        return results

    def build(s):
        q_low, q = in_step(
            stages((LOW0, LOW1)[s], s, 2 * me - 1 + s), stages((UP0, UP1)[s], s, 2 * me - 2 + s)
        )
        lower_high[s], lower_low[s] = split(q_low[bw:])
        mixed = dot3(split(q[:, bw:]), split(q_low[:bw]))
        upper_high[s, :, :bw], upper_low[s, :, :bw] = split(q[:, :bw])
        upper_high[s, :, bw:], upper_low[s, :, bw:] = split(mixed)

        @pl.when(even & inner)
        def _():
            cross[s] = mixed[:bw, bw:]
            across(s).start()

    def across(s):
        return pltpu.make_async_remote_copy(
            src_ref=cross.at[s], dst_ref=crossed.at[s],
            send_sem=cross_send.at[s], recv_sem=cross_recv.at[s],
            device_id={"row": me + 1}, device_id_type=MESH,
        )

    get_hops(EXTRA, ring - 2, last)

    @pl.when(last)
    def _():
        extra_high[...], extra_low[...] = split(in_step(stages(EXTRA, 0, 2 * me))[0])

    def own(q):
        both = dot3((extra_high[...], extra_low[...]), split(x_ref[:, broad(q)]))
        below[0, q], below[1, q] = both[:bw], both[bw:]

    get_hops(LOW0, ring - 2, inner)

    get_hops(UP0, ring - 2, inner)
    steps = 2 * (ring - 1)

    @pl.when(jnp.logical_not(early))
    def _():
        for k in range(steps - 2):
            second(k)

    @pl.when(inner)
    def _():
        build(0)

    @pl.when(ahead)
    def _():
        for k in range(steps - 2, steps):
            second(k)

    @pl.when(ahead)
    def _():
        build(1)

    def up(s, p):
        block = (s, p // 2, slice(None), lanes(p))
        return pltpu.make_async_remote_copy(
            src_ref=tops.at[block], dst_ref=below.at[block],
            send_sem=up_send.at[s, p], recv_sem=up_recv.at[s, p],
            device_id={"row": me - 2}, device_id_type=MESH,
        )

    def over(s, p):
        block = (s, p // 2, slice(None), lanes(p))
        return pltpu.make_async_remote_copy(
            src_ref=partner.at[block], dst_ref=below.at[block],
            send_sem=over_send.at[s, p], recv_sem=over_recv.at[s, p],
            device_id={"row": me - 1}, device_id_type=MESH,
        )

    def near(s, q):
        return pltpu.make_async_remote_copy(
            src_ref=partner.at[s, q], dst_ref=nearby.at[s, q],
            send_sem=near_send.at[s, q], recv_sem=near_recv.at[s, q],
            device_id={"row": me + 1}, device_id_type=MESH,
        )

    def get_initial(q):
        for h in range(2):
            for i in range(2):
                initial(h, 2 * q + i).wait_recv()

    odd_places = ((0, 0), (0, 1), (1, 0), (1, 1), (2, 1))
    even_places = ((1, 1), (2, 1), (3, 0), (3, 0), (3, 0))
    placed = min(steps - 1, len(odd_places)) if pairs >= 4 else 0

    def build_at(q, when):
        @pl.when((q == pairs - 1) & early & when)
        def _():
            for k in range(placed + 1, steps):
                second(k)

        @pl.when((q == pairs - 1) & when)
        def _():
            build(1)

    def second_at(places, q, place):
        for k in range(2):
            @pl.when(jnp.logical_not(early | ahead) & (q == places[k][0]))
            def _():
                if places[k][1] == place:
                    second(steps - 2 + k)

        for k in range(placed):
            if places[k][1] == place:
                @pl.when(early & (q == places[k][0]))
                def _():
                    second(k + 1)

    def share(s, q):
        parts = split(jnp.concatenate([window[0, q], window[1, q]], axis=0))
        return dot3((upper_high[s, :bw, :2 * bw], upper_low[s, :bw, :2 * bw]), parts)

    def settle(s, q):
        parts = split(jnp.concatenate([window[0, q], window[1, q], below[s, q]], axis=0))
        kept = dot3((upper_high[s, bw:], upper_low[s, bw:]), parts)
        ended = dot3((lower_high[s], lower_low[s]), tuple(value[bw:] for value in parts))
        if s == 0:
            window[0, q], window[1, q] = kept, ended
        else:
            out_ref[:bw, broad(q)], out_ref[bw:, broad(q)] = kept, ended

    def carries(s, q, half_lanes):
        step = (upper_high[s, :bw, 2 * bw:], upper_low[s, :bw, 2 * bw:])
        partner[s, q, :, half_lanes] = local[:, half_lanes] + dot3(
            step, split(below[s, q, :, half_lanes])
        )

    def leaving(s, q, half_lanes):
        onward = dot3((cross_high[s], cross_low[s]), split(partner[s, q, :, half_lanes]))
        tops[s, q, :, half_lanes] = nearby[s, q, :, half_lanes] + onward

    def odd_sweep(s):
        def pair(q, carry):
            if s == 0:
                get_initial(q)
            local[...] = share(s, q)

            @pl.when((q == 0) & (me > 1))
            def _():
                across(s).wait_recv()
                cross_high[s], cross_low[s] = split(crossed[s])

            @pl.when(last)
            def _():
                if s == 0:
                    own(q)
                carries(s, q, slice(None))
                near(s, q).wait_recv()
                leaving(s, q, slice(None))
                for i in range(2):
                    up(s, 2 * q + i).start()
                    over(s, 2 * q + i).start()

            @pl.when((me > 1) & jnp.logical_not(last))
            def _():
                near(s, q).wait_recv()

            @pl.when(jnp.logical_not(last))
            def _():
                for i in range(2):
                    p = 2 * q + i
                    half_lanes = slice(i * width, (i + 1) * width)
                    up(s, p).wait_recv()
                    carries(s, q, half_lanes)

                    @pl.when(me > 1)
                    def _():
                        leaving(s, q, half_lanes)
                        up(s, p).start()

                    over(s, p).start()

            if s == 0:
                second_at(odd_places, q, 0)
                build_at(q, jnp.logical_not(ahead))
            settle(s, q)
            if s == 0:
                second_at(odd_places, q, 1)
            return carry

        lax.fori_loop(0, pairs, pair, 0)

    def give(s, q):
        partner[s, q] = share(s, q)
        near(s, q).start()

    def even_sweep(s):
        def pair(q, carry):
            if s == 0:
                second_at(even_places, q, 0)

            if s == 0:
                @pl.when((q < pairs) & inner)
                def _():
                    get_initial(q)
                    give(0, q)

            if s == 0:
                second_at(even_places, q, 1)
                build_at(q, jnp.logical_not(ahead))

                @pl.when((q == pairs) & inner & jnp.logical_not(ahead))
                def _():
                    lax.fori_loop(0, pairs - 1, lambda r, nothing: (give(1, r), nothing)[1], 0)

            @pl.when(q >= 1)
            def _():
                over(s, 2 * q - 2).wait_recv()
                over(s, 2 * q - 1).wait_recv()
                if s == 1:
                    settle(s, q - 1)

            if s == 0:
                @pl.when((q >= 1) & inner)
                def _():
                    settle(s, q - 1)

                @pl.when((q >= 1) & inner & (ahead | (q == pairs)))
                def _():
                    give(1, q - 1)

                @pl.when((q >= 1) & first)
                def _():
                    window[1, q - 1] = below[0, q - 1]

            return carry

        lax.fori_loop(0, pairs + 1, pair, 0)

    def sweep(s):
        @pl.when(odd)
        def _():
            odd_sweep(s)

        @pl.when(even)
        def _():
            even_sweep(s)

    @pl.when(early)
    def _():
        second(0)

    sweep(0)
    sweep(1)

    for slot, when in ((LOW0, inner), (UP0, inner), (LOW1, always), (UP1, always), (EXTRA, last)):
        for t in range(ring - 1):
            for way in range(2):
                @pl.when(when & sends(way, t))
                def _():
                    hop(way, slot, t, slab).wait_send()

    @pl.when(jnp.logical_not(last))
    def _():
        for k in range(len(moved)):
            shift(k).wait_send()

    @pl.when(even & inner)
    def _():
        across(0).wait_send()
        across(1).wait_send()

    def finish(p, carry):
        for s in range(2):
            @pl.when(odd & (me > 1))
            def _():
                up(s, p).wait_send()

            @pl.when(odd)
            def _():
                over(s, p).wait_send()

            @pl.when(even & inner & (p < pairs))
            def _():
                near(s, p).wait_send()

        @pl.when(jnp.logical_not(last))
        def _():
            initial(0, p).wait_send()
            initial(1, p).wait_send()

        return carry

    lax.fori_loop(0, pieces, finish, 0)


def per_device(singular_vectors, reflector_vectors, reflector_factors, sweep_bounds):
    count, ring = lax.axis_size("row"), lax.axis_size("col")
    rows, cols = singular_vectors.shape
    sweeps, blocks, _, span = reflector_vectors.shape
    bw = span // 2
    assert sweeps == 2 and blocks == 2 and rows == span and cols % (2 * WIDTH) == 0
    pairs = cols // (2 * WIDTH)
    assert count % 2 == 0 and count >= 4 and bw == 4 * NEAR and ring >= 2 and pairs >= 2
    vmem, dma = pltpu.VMEM, pltpu.SemaphoreType.DMA
    return pl.pallas_call(
        functools.partial(kernel, count, ring),
        out_shape=jax.ShapeDtypeStruct((rows, cols), f32),
        in_specs=[pl.BlockSpec(memory_space=pltpu.SMEM)] + [pl.BlockSpec(memory_space=pltpu.HBM)] * 3,
        out_specs=pl.BlockSpec(memory_space=vmem),
        scratch_shapes=[
            vmem((rows, cols), f32), vmem(reflector_vectors.shape, f32),
            vmem(reflector_factors.shape, f32), dma((3,)),
            vmem((3, bw, bw + 2 * NEAR), f32), vmem((2, bw, bw), f32),
            vmem((2, bw // ring, bw + 2 * NEAR), f32), vmem((bw // ring, bw), f32),
            vmem((2, span, 3 * bw), bf16), vmem((2, span, 3 * bw), bf16),
            vmem((2, bw, span), bf16), vmem((2, bw, span), bf16),
            vmem((span, span), bf16), vmem((span, span), bf16),
            vmem((2, bw, bw), f32), vmem((2, bw, bw), f32),
            vmem((2, bw, bw), bf16), vmem((2, bw, bw), bf16),
            vmem((2, pairs, bw, 2 * WIDTH), f32),
            vmem((2, pairs, bw, 2 * WIDTH), f32),
            vmem((2, pairs, bw, 2 * WIDTH), f32),
            vmem((2, pairs, bw, 2 * WIDTH), f32),
            vmem((2, pairs, bw, 2 * WIDTH), f32),
            vmem((bw, 2 * WIDTH), f32),
            dma((3,)), dma((3,)), dma((2, 5, ring)), dma((2, 5, ring)),
            dma((2,)), dma((2,)),
            dma((2, 2 * pairs)), dma((2, 2 * pairs)), dma((2, 2 * pairs)), dma((2, 2 * pairs)),
            dma((2, 2 * pairs)), dma((2, 2 * pairs)), dma((2, pairs)), dma((2, pairs)),
        ],
        compiler_params=pltpu.CompilerParams(
            collective_id=0, has_side_effects=True, vmem_limit_bytes=56 * 2**20
        ),
    )(sweep_bounds, singular_vectors, reflector_vectors, reflector_factors)


def solution(mesh):
    placed = (P("row", "col"), P(None, "row", "col", None), P(None, "row", "col", None), P())
    return jax.shard_map(
        per_device, mesh=mesh, in_specs=placed, out_specs=P("row", "col"), check_vma=False
    )
```
